512 devices in a mesh: rows: 32 (over z, core), ch: 16 (over y, x).
Axes of the slice: x: 4, y: 4, z: 16, core: 2. Of those that a mesh axis runs over, the one named last changes fastest.
Arguments:
- features: bfloat16 [128, 256, 8192], P('rows', None, 'ch'), may hold values from -6 to 6
- conv_weight: bfloat16 [3, 3, 256, 256], P(None, None, 'ch'), may hold values from -0.125 to 0.125
- cotangent: bfloat16 [128, 256, 8192], P('rows', None, 'ch'), may hold values from -6 to 6
- valid_rows: int32 [64], replicated, may hold values from 64 to 128
Outputs:
- input_grad: bfloat16 [128, 256, 8192], P('rows', None, 'ch')
- weight_grad: float32 [3, 3, 256, 256], P(None, None, 'ch')
The draws below stay inside these ranges and needn't reach their ends.
All inputs are finite; a program needn't handle non-finite values.
Results may differ from the reference program's by a relative error of at most 0.0049.
Values may be sent and summed in bfloat16 or wider, within the bound.
No kernel may reach another device: no remote copies, remote signals or barrier semaphores. Data moves between devices by JAX's collectives and lax.ppermute only.
A program may use at most 64 MiB of HBM per device.

```python
import jax
import jax.numpy as jnp
from jax import lax

C = 256
COLS = 128
IMAGES = 64
H = 128


def place_ends(drawn, own_key, low, top_value):
    extent = drawn.shape
    place = [jax.random.randint(jax.random.fold_in(own_key, axis), (), 0, extent[axis]) for axis in range(len(extent))]
    drawn = drawn.at[tuple(place)].set(low)
    longest = extent.index(max(extent))
    place[longest] = (place[longest] + 1) % extent[longest]
    return drawn.at[tuple(place)].set(top_value)


def block_levels(own_key, dims, cuts, low, high):
    def one(dim, parts):
        steps = jax.random.uniform(jax.random.fold_in(jax.random.fold_in(own_key, 6), dim), (parts,), jnp.float32, low / len(cuts), high / len(cuts))
        return jnp.repeat(jnp.exp(steps), dims[dim] // parts).reshape((-1,) + (1,) * (len(dims) - dim - 1))

    gain = one(*cuts[0])
    for cut in cuts[1:]:
        gain = gain * one(*cut)
    return gain


def scatter_about(own_key, shape, scale, bound, cuts=(), kind=jnp.bfloat16):
    result = jax.random.normal(own_key, shape, jnp.float32) * scale
    if len(cuts) > 0:
        result = block_levels(own_key, shape, cuts, -0.22, 0.18) * result
    return jnp.clip(result, min=-bound, max=bound).astype(kind)


def setup_inputs(seed: int = 0) -> dict:
    key_of = jax.random.split(jax.random.key(seed), 5)
    return {
        "features": scatter_about(key_of[0], (H, C, IMAGES * COLS), 1.0, 6.0, ((0, 32), (2, 16))),
        "conv_weight": scatter_about(key_of[1], (3, 3, C, C), (9 * C) ** -0.5, 0.125, ((2, 16),)),
        "cotangent": scatter_about(key_of[2], (H, C, IMAGES * COLS), 1.0, 6.0, ((0, 32), (2, 16))),
        "valid_rows": place_ends(jax.random.randint(key_of[3], (IMAGES,), H // 2, H + 1), jax.random.fold_in(key_of[3], 1), H // 2, H).astype(jnp.int32),
    }


def shift_cols(field, across, columns):
    if across == 0:
        return field
    length = field.shape[-1]
    widths = [(0, 0)] * (field.ndim - 1) + [(1, 1)]
    padded = jnp.pad(field, widths)
    moved = padded[..., 1 + across:1 + across + length]
    position = jnp.arange(length).astype(jnp.int32) % columns + across
    inside = (position >= 0) & (position < columns)
    return jnp.where(inside, moved, jnp.zeros_like(moved))

def shifted(field, down, across, columns):
    height = field.shape[0]
    widths = [(1, 1)] + [(0, 0)] * (field.ndim - 1)
    padded = jnp.pad(field, widths)
    return shift_cols(padded[1 + down:1 + down + height], across, columns)

def reference(features, conv_weight, cotangent, valid_rows):
    kernel = conv_weight.astype(jnp.float32)
    feat_images = features.reshape((H, C, IMAGES, COLS)).transpose((2, 0, 1, 3))
    cot_images = cotangent.reshape((H, C, IMAGES, COLS)).transpose((2, 0, 1, 3))

    def per_image(carry, item):
        feat, cot, limit = item
        inputs = feat.astype(jnp.float32)
        summed = jnp.zeros(inputs.shape, jnp.float32)
        for offset_row in range(3):
            for offset_col in range(3):
                summed = summed + jnp.einsum('hik,oi->hok', shifted(inputs, offset_row - 1, offset_col - 1, COLS), kernel[offset_row, offset_col])
        center = lax.optimization_barrier(jnp.sum(summed, 1)) / C
        spread = lax.optimization_barrier(jnp.sum(summed * summed, 1)) / C - center * center
        inverse = lax.rsqrt(spread + 1e-06)
        normed = (summed - center[:, None, :]) * inverse[:, None, :]
        row_ids = jnp.arange(H).astype(jnp.int32)
        keep = (row_ids < limit).astype(jnp.float32)
        masked = cot.astype(jnp.float32) * keep[:, None, None]
        grad_mean = lax.optimization_barrier(jnp.sum(masked, 1)) / C
        grad_cross = lax.optimization_barrier(jnp.sum(masked * normed, 1)) / C
        grad_pre = (inverse[:, None, :] * (masked - grad_mean[:, None, :] - normed * grad_cross[:, None, :])).astype(jnp.bfloat16)
        grad_float = grad_pre.astype(jnp.float32)
        taps = []
        input_sum = jnp.zeros(inputs.shape, jnp.float32)
        for offset_row in range(3):
            for offset_col in range(3):
                taps.append(jnp.einsum('hik,hok->oi', shifted(inputs, offset_row - 1, offset_col - 1, COLS), grad_float))
                input_sum = input_sum + jnp.einsum('hok,oi->hik', shifted(grad_float, 1 - offset_row, 1 - offset_col, COLS), kernel[offset_row, offset_col])
        return (carry + jnp.stack(taps), input_sum.astype(jnp.bfloat16))
    start = jnp.zeros((9, C, C), jnp.float32)
    weight_total, grads = lax.scan(per_image, start, (feat_images, cot_images, valid_rows))
    input_grad = grads.transpose((1, 2, 0, 3)).reshape((H, C, IMAGES * COLS))
    return (input_grad, weight_total.reshape((3, 3, C, C)))
```

```python
import jax
import jax.numpy as jnp
from jax import lax
from jax.experimental import pallas as pl
from jax.experimental.pallas import tpu as pltpu
from jax.sharding import Mesh
from jax.sharding import PartitionSpec as P

COLS = 128
CH = ("ch_0", "ch_1")
ROWS = ("rows_0", "rows_1")
BF16 = jnp.bfloat16
F32 = jnp.float32


def dot(a, b, dims):
    return lax.dot_general(a, b, (dims, ((), ())), preferred_element_type=F32)


def side_shift(tile, across):
    lane = lax.broadcasted_iota(jnp.int32, tile.shape, 1)
    wide = tile.astype(F32)
    moved = pltpu.roll(wide, -across % COLS, 1)
    edge = COLS - 1 if across > 0 else 0
    return jnp.where(lane == edge, 0.0, moved).astype(tile.dtype)


def fill_shifted(out_ref, row, source):
    cells = source.shape[1]
    base = row * cells
    out_ref[1, :, pl.ds(base, cells)] = source
    for image in range(cells // COLS):
        tile = source[:, image * COLS : (image + 1) * COLS]
        for side in (0, 2):
            out_ref[side, :, pl.ds(base + image * COLS, COLS)] = side_shift(tile, side - 1)


def grad_kernel(limits_ref, core_ref, low_ref, feat_ref, high_ref, w_ref, cot_ref,
                grad_ref, own_ref, other_ref, shifted_ref, flat_ref):
    band, ch, cells = feat_ref.shape
    images = cells // COLS
    fill_shifted(shifted_ref, 0, low_ref[0])
    for h in range(band):
        fill_shifted(shifted_ref, h + 1, feat_ref[h])
    fill_shifted(shifted_ref, band + 1, high_ref[0])
    for h in range(band):
        summed = None
        for r in range(3):
            for c in range(3):
                w = w_ref[:, 3 * r + c].reshape(ch, ch)
                x = shifted_ref[c, :, pl.ds((h + r) * cells, cells)]
                term = dot(w, x, ((1,), (0,)))
                summed = term if summed is None else summed + term
        center = jnp.sum(summed, 0, keepdims=True) / ch
        spread = jnp.sum(summed * summed, 0, keepdims=True) / ch - center * center
        inverse = lax.rsqrt(spread + 1e-06)
        normed = (summed - center) * inverse
        keep = jnp.concatenate(
            [jnp.full((1, COLS), jnp.where(h < limits_ref[n], 1.0, 0.0), F32) for n in range(images)], 1
        )
        masked = cot_ref[h].astype(F32) * keep
        total = jnp.sum(masked, 0, keepdims=True) / ch
        cross = jnp.sum(masked * normed, 0, keepdims=True) / ch
        grad = (inverse * (masked - total - normed * cross)).astype(BF16)
        grad_ref[h] = grad
        flat_ref[:, pl.ds(h * cells, cells)] = grad
    half = ch // 2
    first = core_ref[0] == 0
    for r in range(3):
        for c in range(3):
            tap = dot(
                flat_ref[...], shifted_ref[c, :, pl.ds(r * cells, band * cells)], ((1,), (1,))
            )
            left, right = tap[:, :half], tap[:, half:]
            parts = own_ref.shape[0], own_ref.shape[2], half
            own_ref[:, 3 * r + c] = jnp.where(first, left, right).reshape(parts)
            other_ref[:, 3 * r + c] = jnp.where(first, right, left).astype(BF16).reshape(parts)


def input_kernel(low_ref, grad_ref, high_ref, w_ref, out_ref, shifted_ref, wt_ref):
    band, ch, cells = grad_ref.shape
    fill_shifted(shifted_ref, 0, low_ref[0])
    for h in range(band):
        fill_shifted(shifted_ref, h + 1, grad_ref[h])
    fill_shifted(shifted_ref, band + 1, high_ref[0])
    for t in range(9):
        wt_ref[t] = w_ref[:, t].reshape(ch, ch).T
    for h in range(band):
        summed = None
        for r in range(3):
            for c in range(3):
                x = shifted_ref[2 - c, :, pl.ds((h + 2 - r) * cells, cells)]
                term = dot(wt_ref[3 * r + c], x, ((1,), (0,)))
                summed = term if summed is None else summed + term
        out_ref[h] = summed.astype(BF16)


def exchange(block, axis):
    return lax.ppermute(block, axis, [(0, 1), (1, 0)])


def band_edges(block):
    count = lax.axis_size(ROWS)
    forward = [(i, i + 1) for i in range(count - 1)]
    backward = [(target, source) for source, target in forward]
    low = lax.ppermute(block[-1:], ROWS, forward)
    high = lax.ppermute(block[:1], ROWS, backward)
    return low, high


def to_all(block, axis):
    peers = lax.axis_size(axis)
    return lax.all_to_all(jnp.broadcast_to(block[None], (peers, *block.shape)), axis, 0, 0, tiled=True)


def vmem(count):
    return [pl.BlockSpec(memory_space=pltpu.VMEM)] * count


def work(block, convs):
    band, ch, cells = block.shape
    return pl.CostEstimate(
        flops=convs * 18 * ch * ch * band * cells, bytes_accessed=convs << 22, transcendentals=0
    )


def call_grad(limits, core, low, features, high, kernel, cotangent):
    band, ch, cells = features.shape
    halved = (*kernel.shape[:3], ch // 2)
    return pl.pallas_call(
        grad_kernel,
        in_specs=[pl.BlockSpec(memory_space=pltpu.SMEM)] * 2 + vmem(5),
        out_specs=vmem(3),
        out_shape=[
            jax.ShapeDtypeStruct(features.shape, BF16),
            jax.ShapeDtypeStruct(halved, F32),
            jax.ShapeDtypeStruct(halved, BF16),
        ],
        scratch_shapes=[
            pltpu.VMEM((3, ch, (band + 2) * cells), BF16),
            pltpu.VMEM((ch, band * cells), BF16),
        ],
        cost_estimate=work(features, 2),
        compiler_params=pltpu.CompilerParams(vmem_limit_bytes=24 << 20),
        name="grad",
    )(limits, core, low, features, high, kernel, cotangent)


def call_input(low, grad, high, kernel):
    band, ch, cells = grad.shape
    return pl.pallas_call(
        input_kernel,
        in_specs=vmem(4),
        out_specs=vmem(1)[0],
        out_shape=jax.ShapeDtypeStruct(grad.shape, BF16),
        scratch_shapes=[
            pltpu.VMEM((3, ch, (band + 2) * cells), BF16),
            pltpu.VMEM((9, ch, ch), BF16),
        ],
        cost_estimate=work(grad, 1),
        compiler_params=pltpu.CompilerParams(vmem_limit_bytes=20 << 20),
        name="input",
    )(low, grad, high, kernel)


def body(features, conv_weight, cotangent, valid_rows):
    band, ch, cells = features.shape
    images = cells // COLS
    near = conv_weight.shape[2]
    half = ch // 2
    core = lax.axis_index("rows_1").astype(jnp.int32).reshape(1)
    limits = lax.dynamic_slice_in_dim(valid_rows, lax.axis_index(CH) * images, images, 0)
    limits = limits - lax.axis_index(ROWS) * band
    kernel = to_all(conv_weight.reshape(9, near, ch), CH)
    low, high = band_edges(features)
    grad_pre, own, other = call_grad(limits, core, low, features, high, kernel, cotangent)
    pair = (own + exchange(other, "rows_1").astype(F32)).astype(BF16)
    plane = lax.all_to_all(pair, CH, 0, 0, tiled=True).astype(F32).sum(0)
    lines = plane.transpose(1, 0, 2)
    share = lax.all_to_all(lines, "rows_0", 0, 0, tiled=True).reshape(near, 9, half).sum(0)
    mine = to_all(share, "rows_0")
    theirs = exchange(mine, "rows_1")
    first = core[0] == 0
    weight_grad = jnp.concatenate(
        [jnp.where(first, mine, theirs), jnp.where(first, theirs, mine)], 2
    ).transpose(1, 0, 2)
    grad_low, grad_high = band_edges(grad_pre)
    input_grad = call_input(grad_low, grad_pre, grad_high, kernel)
    return input_grad, weight_grad.reshape(3, 3, near, ch)


def solution(mesh):
    split = Mesh(mesh.devices.reshape(16, 2, 4, 4), ("rows_0", "rows_1", "ch_0", "ch_1"))
    placed = (P(ROWS, None, CH), P(None, None, CH, None), P(ROWS, None, CH), P())
    return jax.shard_map(
        body,
        mesh=split,
        in_specs=placed,
        out_specs=(P(ROWS, None, CH), P(None, None, CH, None)),
        check_vma=False,
    )
```

```python
import jax
import jax.numpy as jnp
from jax import lax
from jax.experimental import pallas as pl
from jax.experimental.pallas import tpu as pltpu
from jax.sharding import Mesh
from jax.sharding import PartitionSpec as P

COLS = 128
CH = ("ch_0", "ch_1")
ROWS = ("z_far", "z_near", "core")
BF16 = jnp.bfloat16
F32 = jnp.float32


def dot(a, b, dims):
    return lax.dot_general(a, b, (dims, ((), ())), preferred_element_type=F32)


def side_shift(tile, across):
    lane = lax.broadcasted_iota(jnp.int32, tile.shape, 1)
    moved = pltpu.roll(tile.astype(F32), -across % COLS, 1)
    edge = COLS - 1 if across > 0 else 0
    return jnp.where(lane == edge, 0.0, moved).astype(tile.dtype)


def fill_shifted(out_ref, row, halves):
    half, cells = halves[0].shape
    for k, source in enumerate(halves):
        rows = slice(k * half, (k + 1) * half)
        out_ref[1, rows, pl.ds(row * cells, cells)] = source
        for image in range(cells // COLS):
            tile = source[:, image * COLS : (image + 1) * COLS]
            for side in (0, 2):
                out_ref[side, rows, pl.ds(row * cells + image * COLS, COLS)] = side_shift(tile, side - 1)


def grad_kernel(limits_ref, core_ref, low_hbm, feat_hbm, high_hbm, mine_ref, theirs_ref, cot_hbm,
                grad_ref, own_ref, other_ref, feat_ref, cot_ref, shifted_ref, flat_ref, sems):
    band, ch, cells = cot_ref.shape
    images = cells // COLS
    half = ch // 2
    sources = [low_hbm.at[0]] + [feat_hbm.at[h] for h in range(band)] + [high_hbm.at[0]]
    loads = [pltpu.make_async_copy(s, feat_ref.at[h], sems.at[h]) for h, s in enumerate(sources)]
    masks = [
        pltpu.make_async_copy(cot_hbm.at[h], cot_ref.at[h], sems.at[band + 2 + h]) for h in range(band)
    ]
    for load in loads + masks:
        load.start()
    near = pl.ds(pl.multiple_of(core_ref[0] * half, half), half)
    far = pl.ds(pl.multiple_of((1 - core_ref[0]) * half, half), half)
    for h in range(band + 2):
        loads[h].wait()
        fill_shifted(shifted_ref, h, [feat_ref[h, near], feat_ref[h, far]])
    for h in range(band):
        summed = None
        for r in range(3):
            for c in range(3):
                t = 3 * r + c
                w = jnp.concatenate(
                    [mine_ref[:, t].reshape(ch, half), theirs_ref[:, t].reshape(ch, half)], 1
                )
                x = shifted_ref[c, :, pl.ds((h + r) * cells, cells)]
                term = dot(w, x, ((1,), (0,)))
                summed = term if summed is None else summed + term
        center = jnp.sum(summed, 0, keepdims=True) / ch
        spread = jnp.sum(summed * summed, 0, keepdims=True) / ch - center * center
        inverse = lax.rsqrt(spread + 1e-06)
        normed = (summed - center) * inverse
        keep = jnp.concatenate(
            [jnp.full((1, COLS), jnp.where(h < limits_ref[n], 1.0, 0.0), F32) for n in range(images)], 1
        )
        masks[h].wait()
        masked = cot_ref[h].astype(F32) * keep
        total = jnp.sum(masked, 0, keepdims=True) / ch
        cross = jnp.sum(masked * normed, 0, keepdims=True) / ch
        grad = (inverse * (masked - total - normed * cross)).astype(BF16)
        grad_ref[h] = grad
        flat_ref[:, pl.ds(h * cells, cells)] = grad
    parts = own_ref.shape[0], own_ref.shape[2], half
    for r in range(3):
        for c in range(3):
            t = 3 * r + c
            tap = dot(flat_ref[...], shifted_ref[c, :, pl.ds(r * cells, band * cells)], ((1,), (1,)))
            own_ref[:, t] = tap[:, :half].reshape(parts)
            other_ref[:, t] = tap[:, half:].astype(BF16).reshape(parts)


def input_kernel(core_ref, low_ref, grad_ref, high_ref, mine_ref, theirs_ref, out_ref, shifted_ref, wt_ref):
    band, ch, cells = grad_ref.shape
    half = ch // 2
    near = pl.ds(pl.multiple_of(core_ref[0] * half, half), half)
    far = pl.ds(pl.multiple_of((1 - core_ref[0]) * half, half), half)
    fill_shifted(shifted_ref, 0, [low_ref[0]])
    for h in range(band):
        fill_shifted(shifted_ref, h + 1, [grad_ref[h]])
    fill_shifted(shifted_ref, band + 1, [high_ref[0]])
    for t in range(9):
        wt_ref[t, :half] = mine_ref[:, t].reshape(ch, half).T
        wt_ref[t, half:] = theirs_ref[:, t].reshape(ch, half).T
    for h in range(band):
        summed = None
        for r in range(3):
            for c in range(3):
                x = shifted_ref[2 - c, :, pl.ds((h + 2 - r) * cells, cells)]
                term = dot(wt_ref[3 * r + c], x, ((1,), (0,)))
                summed = term if summed is None else summed + term
        out_ref[h, near] = summed[:half].astype(BF16)
        out_ref[h, far] = summed[half:].astype(BF16)


def vmem(count):
    return [pl.BlockSpec(memory_space=pltpu.VMEM)] * count


def smem(count):
    return [pl.BlockSpec(memory_space=pltpu.SMEM)] * count


def in_hbm(block):
    return pltpu.with_memory_space_constraint(block, pltpu.HBM)


HBM = pl.BlockSpec(memory_space=pltpu.HBM)


def work(block, convs):
    band, ch, cells = block.shape
    return pl.CostEstimate(
        flops=convs * 18 * ch * ch * band * cells, bytes_accessed=convs << 22, transcendentals=0
    )


def call_grad(limits, core, low, features, high, mine, theirs, cotangent):
    band, ch, cells = features.shape
    return pl.pallas_call(
        grad_kernel,
        in_specs=smem(2) + [HBM] * 3 + vmem(2) + [HBM],
        out_specs=vmem(3),
        out_shape=[
            jax.ShapeDtypeStruct(features.shape, BF16),
            jax.ShapeDtypeStruct(mine.shape, F32),
            jax.ShapeDtypeStruct(mine.shape, BF16),
        ],
        scratch_shapes=[
            pltpu.VMEM((band + 2, ch, cells), BF16),
            pltpu.VMEM(features.shape, BF16),
            pltpu.VMEM((3, ch, (band + 2) * cells), BF16),
            pltpu.VMEM((ch, band * cells), BF16),
            pltpu.SemaphoreType.DMA((2 * band + 2,)),
        ],
        cost_estimate=work(features, 2),
        compiler_params=pltpu.CompilerParams(vmem_limit_bytes=24 << 20),
        name="grad",
    )(limits, core, *map(in_hbm, (low, features, high)), mine, theirs, in_hbm(cotangent))


def call_input(core, low, grad, high, mine, theirs):
    band, ch, cells = grad.shape
    return pl.pallas_call(
        input_kernel,
        in_specs=smem(1) + vmem(5),
        out_specs=vmem(1)[0],
        out_shape=jax.ShapeDtypeStruct(grad.shape, BF16),
        scratch_shapes=[
            pltpu.VMEM((3, ch, (band + 2) * cells), BF16),
            pltpu.VMEM((9, ch, ch), BF16),
        ],
        cost_estimate=work(grad, 1),
        compiler_params=pltpu.CompilerParams(vmem_limit_bytes=20 << 20),
        name="input",
    )(core, low, grad, high, mine, theirs)


def exchange(block):
    return lax.ppermute(block, "core", [(0, 1), (1, 0)])


def band_edges(block):
    count = lax.axis_size(ROWS)
    forward = [(i, i + 1) for i in range(count - 1)]
    backward = [(target, source) for source, target in forward]
    low = lax.ppermute(block[-1:], ROWS, forward)
    high = lax.ppermute(block[:1], ROWS, backward)
    return low, high


def to_all(block, axis):
    peers = lax.axis_size(axis)
    return lax.all_to_all(jnp.broadcast_to(block[None], (peers, *block.shape)), axis, 0, 0, tiled=True)


def body(features, conv_weight, cotangent, valid_rows):
    band, ch, cells = features.shape
    images = cells // COLS
    near = conv_weight.shape[2]
    half = ch // 2
    core = lax.axis_index("core").astype(jnp.int32)
    limits = lax.dynamic_slice_in_dim(valid_rows, lax.axis_index(CH) * images, images, 0)
    limits = limits - lax.axis_index(ROWS) * band
    share = lax.dynamic_slice_in_dim(conv_weight, core * half, half, 3).reshape(9, near, half)
    mine = to_all(share, CH)
    low, high = band_edges(features)
    mine, low, high = lax.optimization_barrier((mine, low, high))
    theirs = exchange(mine)
    core = core.reshape(1)
    grad_pre, own, other = call_grad(limits, core, low, features, high, mine, theirs, cotangent)
    grad_low, grad_high = band_edges(grad_pre)
    pair = (own + exchange(other).astype(F32)).astype(BF16)
    plane = lax.all_to_all(pair, CH, 0, 0, tiled=True)
    plane, grad_low, grad_high = lax.optimization_barrier((plane, grad_low, grad_high))
    input_grad = call_input(core, grad_low, grad_pre, grad_high, mine, theirs)
    plane = plane.astype(F32).sum(0)
    lines = plane.reshape(lax.axis_size("z_near"), -1, half)
    block = lax.all_to_all(lines, "z_near", 0, 0, tiled=True).sum(0)
    block, input_grad = lax.optimization_barrier((to_all(block, "z_far"), input_grad))
    block = block.sum(0)
    whole = to_all(block, ("z_near", "core")).reshape(-1, 2, *block.shape)
    weight_grad = whole.swapaxes(1, 2).reshape(3, 3, near, ch)
    return input_grad, weight_grad


def solution(mesh):
    names = ("z_far", "z_near", "core", "ch_0", "ch_1")
    split = Mesh(mesh.devices.reshape(4, 4, 2, 4, 4), names)
    placed = (P(ROWS, None, CH), P(None, None, CH, None), P(ROWS, None, CH), P())
    return jax.shard_map(
        body,
        mesh=split,
        in_specs=placed,
        out_specs=(P(ROWS, None, CH), P(None, None, CH, None)),
        check_vma=False,
    )
```

```python
import jax
import jax.numpy as jnp
from jax import lax
from jax.experimental import pallas as pl
from jax.experimental.pallas import tpu as pltpu
from jax.sharding import Mesh
from jax.sharding import PartitionSpec as P

COLS = 128
CH = ("ch_0", "ch_1")
ROWS = ("z_far", "z_near", "core")
BF16 = jnp.bfloat16
F32 = jnp.float32


def dot(a, b, dims):
    return lax.dot_general(a, b, (dims, ((), ())), preferred_element_type=F32)


def side_shift(tile, across):
    lane = lax.broadcasted_iota(jnp.int32, tile.shape, 1)
    moved = pltpu.roll(tile.astype(F32), -across % COLS, 1)
    edge = COLS - 1 if across > 0 else 0
    return jnp.where(lane == edge, 0.0, moved).astype(tile.dtype)


def fill_shifted(out_ref, row, halves):
    half, cells = halves[0].shape
    for k, source in enumerate(halves):
        rows = slice(k * half, (k + 1) * half)
        out_ref[1, rows, pl.ds(row * cells, cells)] = source
        for image in range(cells // COLS):
            tile = source[:, image * COLS : (image + 1) * COLS]
            for side in (0, 2):
                out_ref[side, rows, pl.ds(row * cells + image * COLS, COLS)] = side_shift(tile, side - 1)


def grad_kernel(limits_ref, core_ref, low_hbm, feat_hbm, high_hbm, mine_ref, theirs_ref, cot_hbm,
                grad_ref, own_ref, other_ref, feat_ref, cot_ref, shifted_ref, flat_ref, sems):
    band, ch, cells = cot_ref.shape
    images = cells // COLS
    half = ch // 2
    sources = [low_hbm.at[0]] + [feat_hbm.at[h] for h in range(band)] + [high_hbm.at[0]]
    loads = [pltpu.make_async_copy(s, feat_ref.at[h], sems.at[h]) for h, s in enumerate(sources)]
    masks = [
        pltpu.make_async_copy(cot_hbm.at[h], cot_ref.at[h], sems.at[band + 2 + h]) for h in range(band)
    ]
    for load in loads + masks:
        load.start()
    near = pl.ds(pl.multiple_of(core_ref[0] * half, half), half)
    far = pl.ds(pl.multiple_of((1 - core_ref[0]) * half, half), half)
    for load in loads + masks:
        load.wait()
    for h in range(band + 2):
        fill_shifted(shifted_ref, h, [feat_ref[h, near], feat_ref[h, far]])
    for h in range(band):
        summed = None
        for r in range(3):
            for c in range(3):
                t = 3 * r + c
                w = jnp.concatenate(
                    [mine_ref[:, t].reshape(ch, half), theirs_ref[:, t].reshape(ch, half)], 1
                )
                x = shifted_ref[c, :, pl.ds((h + r) * cells, cells)]
                term = dot(w, x, ((1,), (0,)))
                summed = term if summed is None else summed + term
        center = jnp.sum(summed, 0, keepdims=True) / ch
        spread = jnp.sum(summed * summed, 0, keepdims=True) / ch - center * center
        inverse = lax.rsqrt(spread + 1e-06)
        normed = (summed - center) * inverse
        keep = jnp.concatenate(
            [jnp.full((1, COLS), jnp.where(h < limits_ref[n], 1.0, 0.0), F32) for n in range(images)], 1
        )
        masked = cot_ref[h].astype(F32) * keep
        total = jnp.sum(masked, 0, keepdims=True) / ch
        cross = jnp.sum(masked * normed, 0, keepdims=True) / ch
        grad = (inverse * (masked - total - normed * cross)).astype(BF16)
        grad_ref[h] = grad
        flat_ref[:, pl.ds(h * cells, cells)] = grad
    parts = own_ref.shape[0], own_ref.shape[2], half
    for r in range(3):
        for c in range(3):
            t = 3 * r + c
            tap = dot(flat_ref[...], shifted_ref[c, :, pl.ds(r * cells, band * cells)], ((1,), (1,)))
            own_ref[:, t] = tap[:, :half].reshape(parts)
            other_ref[:, t] = tap[:, half:].astype(BF16).reshape(parts)


def input_kernel(core_ref, low_ref, grad_ref, high_ref, mine_ref, theirs_ref, out_ref, shifted_ref, wt_ref):
    band, ch, cells = grad_ref.shape
    half = ch // 2
    near = pl.ds(pl.multiple_of(core_ref[0] * half, half), half)
    far = pl.ds(pl.multiple_of((1 - core_ref[0]) * half, half), half)
    fill_shifted(shifted_ref, 0, [low_ref[0]])
    for h in range(band):
        fill_shifted(shifted_ref, h + 1, [grad_ref[h]])
    fill_shifted(shifted_ref, band + 1, [high_ref[0]])
    for t in range(9):
        wt_ref[t, :half] = mine_ref[:, t].reshape(ch, half).T
        wt_ref[t, half:] = theirs_ref[:, t].reshape(ch, half).T
    for h in range(band):
        summed = None
        for r in range(3):
            for c in range(3):
                x = shifted_ref[2 - c, :, pl.ds((h + 2 - r) * cells, cells)]
                term = dot(wt_ref[3 * r + c], x, ((1,), (0,)))
                summed = term if summed is None else summed + term
        out_ref[h, near] = summed[:half].astype(BF16)
        out_ref[h, far] = summed[half:].astype(BF16)


def vmem(count):
    return [pl.BlockSpec(memory_space=pltpu.VMEM)] * count


def smem(count):
    return [pl.BlockSpec(memory_space=pltpu.SMEM)] * count


def in_hbm(block):
    return pltpu.with_memory_space_constraint(block, pltpu.HBM)


HBM = pl.BlockSpec(memory_space=pltpu.HBM)


def work(block, convs):
    band, ch, cells = block.shape
    return pl.CostEstimate(
        flops=convs * 18 * ch * ch * band * cells, bytes_accessed=convs << 22, transcendentals=0
    )


def call_grad(limits, core, low, features, high, mine, theirs, cotangent):
    band, ch, cells = features.shape
    return pl.pallas_call(
        grad_kernel,
        in_specs=smem(2) + [HBM] * 3 + vmem(2) + [HBM],
        out_specs=vmem(3),
        out_shape=[
            jax.ShapeDtypeStruct(features.shape, BF16),
            jax.ShapeDtypeStruct(mine.shape, F32),
            jax.ShapeDtypeStruct(mine.shape, BF16),
        ],
        scratch_shapes=[
            pltpu.VMEM((band + 2, ch, cells), BF16),
            pltpu.VMEM(features.shape, BF16),
            pltpu.VMEM((3, ch, (band + 2) * cells), BF16),
            pltpu.VMEM((ch, band * cells), BF16),
            pltpu.SemaphoreType.DMA((2 * band + 2,)),
        ],
        cost_estimate=work(features, 2),
        compiler_params=pltpu.CompilerParams(vmem_limit_bytes=24 << 20),
        name="grad",
    )(limits, core, *map(in_hbm, (low, features, high)), mine, theirs, in_hbm(cotangent))


def call_input(core, low, grad, high, mine, theirs):
    band, ch, cells = grad.shape
    return pl.pallas_call(
        input_kernel,
        in_specs=smem(1) + vmem(5),
        out_specs=vmem(1)[0],
        out_shape=jax.ShapeDtypeStruct(grad.shape, BF16),
        scratch_shapes=[
            pltpu.VMEM((3, ch, (band + 2) * cells), BF16),
            pltpu.VMEM((9, ch, ch), BF16),
        ],
        cost_estimate=work(grad, 1),
        compiler_params=pltpu.CompilerParams(vmem_limit_bytes=20 << 20),
        name="input",
    )(core, low, grad, high, mine, theirs)


def exchange(block):
    return lax.ppermute(block, "core", [(0, 1), (1, 0)])


def band_edges(block):
    count = lax.axis_size(ROWS)
    forward = [(i, i + 1) for i in range(count - 1)]
    backward = [(target, source) for source, target in forward]
    low = lax.ppermute(block[-1:], ROWS, forward)
    high = lax.ppermute(block[:1], ROWS, backward)
    return low, high


def copies(block, axis):
    return jnp.broadcast_to(block[None], (lax.axis_size(axis), *block.shape))


def swap(parts, axis):
    return lax.all_to_all(parts, axis, 0, 0, tiled=True)


def body(features, conv_weight, cotangent, valid_rows):
    band, ch, cells = features.shape
    images = cells // COLS
    near = conv_weight.shape[2]
    half = ch // 2
    core = lax.axis_index("core").astype(jnp.int32)
    limits = lax.dynamic_slice_in_dim(valid_rows, lax.axis_index(CH) * images, images, 0)
    limits = limits - lax.axis_index(ROWS) * band
    share = lax.dynamic_slice_in_dim(conv_weight, core * half, half, 3).reshape(9, near, half)
    low, high = band_edges(features)
    parts, low, high = lax.optimization_barrier((copies(share, CH), low, high))
    mine = swap(parts, CH)
    theirs = exchange(mine)
    core = core.reshape(1)
    grad_pre, own, other = call_grad(limits, core, low, features, high, mine, theirs, cotangent)
    pair = (own + exchange(other).astype(F32)).astype(BF16)
    plane = swap(pair, CH).astype(F32).sum(0)
    lines = plane.reshape(lax.axis_size("z_near"), -1, half)
    block = copies(swap(lines, "z_near").sum(0), "z_far")
    block, grad_pre = lax.optimization_barrier((block, grad_pre))
    grad_low, grad_high = band_edges(grad_pre)
    input_grad = call_input(core, grad_low, grad_pre, grad_high, mine, theirs)
    block = swap(block, "z_far")
    block, input_grad = lax.optimization_barrier((block, input_grad))
    pieces = ("z_near", "core")
    whole = swap(copies(block.sum(0), pieces), pieces).reshape(-1, 2, *block.shape[1:])
    weight_grad = whole.swapaxes(1, 2).reshape(3, 3, near, ch)
    return input_grad, weight_grad


def solution(mesh):
    names = ("z_far", "z_near", "core", "ch_0", "ch_1")
    split = Mesh(mesh.devices.reshape(4, 4, 2, 4, 4), names)
    placed = (P(ROWS, None, CH), P(None, None, CH, None), P(ROWS, None, CH), P())
    return jax.shard_map(
        body,
        mesh=split,
        in_specs=placed,
        out_specs=(P(ROWS, None, CH), P(None, None, CH, None)),
        check_vma=False,
    )
```

```python
import jax
import jax.numpy as jnp
from jax import lax
from jax.experimental import pallas as pl
from jax.experimental.pallas import tpu as pltpu
from jax.sharding import Mesh
from jax.sharding import PartitionSpec as P

COLS = 128
CH = ("ch_0", "ch_1")
ROWS = ("z_far", "z_near", "core")
BF16 = jnp.bfloat16
F32 = jnp.float32


def dot(a, b, dims):
    return lax.dot_general(a, b, (dims, ((), ())), preferred_element_type=F32)


def side_shift(tile, across):
    lane = lax.broadcasted_iota(jnp.int32, tile.shape, 1)
    moved = pltpu.roll(tile.astype(F32), -across % COLS, 1)
    edge = COLS - 1 if across > 0 else 0
    return jnp.where(lane == edge, 0.0, moved).astype(tile.dtype)


def fill_shifted(out_ref, row, halves):
    half, cells = halves[0].shape
    for k, source in enumerate(halves):
        rows = slice(k * half, (k + 1) * half)
        out_ref[1, rows, pl.ds(row * cells, cells)] = source
        for image in range(cells // COLS):
            tile = source[:, image * COLS : (image + 1) * COLS]
            for side in (0, 2):
                out_ref[side, rows, pl.ds(row * cells + image * COLS, COLS)] = side_shift(tile, side - 1)


def grad_kernel(limits_ref, core_ref, inner_hbm, feat_hbm, outer_hbm, mine_ref, theirs_ref, cot_hbm,
                grad_hbm, outer_ref, own_ref, sent_ref,
                feat_ref, cot_ref, shifted_ref, flat_ref, grad_ref, sems):
    band, ch, cells = cot_ref.shape
    images = cells // COLS
    half = ch // 2
    core = core_ref[0]
    rows = [(inner_hbm.at[0], (1 - core) * (band + 1)), (outer_hbm.at[0], core * (band + 1))]
    rows += [(feat_hbm.at[h], h + 1) for h in range(band)]
    copies = [(source, feat_ref.at[row]) for source, row in rows]
    copies += [(cot_hbm.at[h], cot_ref.at[h]) for h in range(band)]
    loads = [pltpu.make_async_copy(src, dst, sems.at[i]) for i, (src, dst) in enumerate(copies)]
    for load in loads:
        load.start()
    near = pl.ds(pl.multiple_of(core * half, half), half)
    far = pl.ds(pl.multiple_of((1 - core) * half, half), half)
    for load in loads:
        load.wait()
    for h in range(band + 2):
        fill_shifted(shifted_ref, h, [feat_ref[h, near], feat_ref[h, far]])
    for h in range(band):
        summed = None
        for r in range(3):
            for c in range(3):
                t = 3 * r + c
                w = jnp.concatenate(
                    [mine_ref[:, t].reshape(ch, half), theirs_ref[:, t].reshape(ch, half)], 1
                )
                x = shifted_ref[c, :, pl.ds((h + r) * cells, cells)]
                term = dot(w, x, ((1,), (0,)))
                summed = term if summed is None else summed + term
        center = jnp.sum(summed, 0, keepdims=True) / ch
        spread = jnp.sum(summed * summed, 0, keepdims=True) / ch - center * center
        inverse = lax.rsqrt(spread + 1e-06)
        normed = (summed - center) * inverse
        keep = jnp.concatenate(
            [jnp.full((1, COLS), jnp.where(h < limits_ref[n], 1.0, 0.0), F32) for n in range(images)], 1
        )
        masked = cot_ref[h].astype(F32) * keep
        total = jnp.sum(masked, 0, keepdims=True) / ch
        cross = jnp.sum(masked * normed, 0, keepdims=True) / ch
        grad = (inverse * (masked - total - normed * cross)).astype(BF16)
        grad_ref[h] = grad
        flat_ref[:, pl.ds(h * cells, cells)] = grad
    parts, taps, near_ch, _ = own_ref.shape
    saves = [pltpu.make_async_copy(grad_ref.at[h], grad_hbm.at[h], sems.at[h]) for h in range(band)]
    for r in range(3):
        for c in range(3):
            t = 3 * r + c
            if t == 1:
                for save in saves:
                    save.start()
            tap = dot(flat_ref[...], shifted_ref[c, :, pl.ds(r * cells, band * cells)], ((1,), (1,)))
            own_ref[:, t] = tap[:, :half].reshape(parts, near_ch, half)
            sent_ref[:parts, t] = tap[:, half:].astype(BF16).reshape(parts, near_ch, half)
    first = core == 0
    bottom, top = grad_ref[0], grad_ref[band - 1]
    outer_ref[0] = jnp.where(first, bottom, top)
    inner = jnp.where(first, top, bottom)
    for g in range(images * parts):
        n, p = divmod(g, parts)
        sent_ref[parts + g // taps, g % taps] = inner[
            p * near_ch : (p + 1) * near_ch, n * COLS : (n + 1) * COLS
        ]
    for save in saves:
        save.wait()


def input_kernel(core_ref, got_ref, grad_ref, outer_ref, mine_ref, theirs_ref, out_ref, shifted_ref, wt_ref):
    band, ch, cells = grad_ref.shape
    half = ch // 2
    first = core_ref[0] == 0
    parts, taps = mine_ref.shape[:2]
    groups = [got_ref[parts + g // taps, g % taps] for g in range(parts * (cells // COLS))]
    images = [jnp.concatenate(groups[k : k + parts], 0) for k in range(0, len(groups), parts)]
    inner = jnp.concatenate(images, 1)
    outer = outer_ref[0]
    near = pl.ds(pl.multiple_of(core_ref[0] * half, half), half)
    far = pl.ds(pl.multiple_of((1 - core_ref[0]) * half, half), half)
    fill_shifted(shifted_ref, 0, [jnp.where(first, outer, inner)])
    for h in range(band):
        fill_shifted(shifted_ref, h + 1, [grad_ref[h]])
    fill_shifted(shifted_ref, band + 1, [jnp.where(first, inner, outer)])
    for t in range(9):
        wt_ref[t, :half] = mine_ref[:, t].reshape(ch, half).T
        wt_ref[t, half:] = theirs_ref[:, t].reshape(ch, half).T
    for h in range(band):
        summed = None
        for r in range(3):
            for c in range(3):
                x = shifted_ref[2 - c, :, pl.ds((h + 2 - r) * cells, cells)]
                term = dot(wt_ref[3 * r + c], x, ((1,), (0,)))
                summed = term if summed is None else summed + term
        out_ref[h, near] = summed[:half].astype(BF16)
        out_ref[h, far] = summed[half:].astype(BF16)


def vmem(count):
    return [pl.BlockSpec(memory_space=pltpu.VMEM)] * count


def smem(count):
    return [pl.BlockSpec(memory_space=pltpu.SMEM)] * count


def in_hbm(block):
    return pltpu.with_memory_space_constraint(block, pltpu.HBM)


HBM = pl.BlockSpec(memory_space=pltpu.HBM)


def work(block, convs):
    band, ch, cells = block.shape
    return pl.CostEstimate(
        flops=convs * 18 * ch * ch * band * cells, bytes_accessed=convs << 22, transcendentals=0
    )


def call_grad(limits, core, inner, features, outer, mine, theirs, cotangent):
    band, ch, cells = features.shape
    parts, taps, _, _ = mine.shape
    edge_parts = pl.cdiv(parts * (cells // COLS), taps)
    return pl.pallas_call(
        grad_kernel,
        in_specs=smem(2) + [HBM] * 3 + vmem(2) + [HBM],
        out_specs=[HBM] + vmem(3),
        out_shape=[
            pltpu.HBM(features.shape, BF16),
            jax.ShapeDtypeStruct(outer.shape, BF16),
            jax.ShapeDtypeStruct(mine.shape, F32),
            jax.ShapeDtypeStruct((parts + edge_parts, *mine.shape[1:]), BF16),
        ],
        scratch_shapes=[
            pltpu.VMEM((band + 2, ch, cells), BF16),
            pltpu.VMEM(features.shape, BF16),
            pltpu.VMEM((3, ch, (band + 2) * cells), BF16),
            pltpu.VMEM((ch, band * cells), BF16),
            pltpu.VMEM(features.shape, BF16),
            pltpu.SemaphoreType.DMA((2 * band + 2,)),
        ],
        cost_estimate=work(features, 2),
        compiler_params=pltpu.CompilerParams(vmem_limit_bytes=24 << 20),
        name="grad",
    )(limits, core, *map(in_hbm, (inner, features, outer)), mine, theirs, in_hbm(cotangent))


def call_input(core, got, grad, outer, mine, theirs):
    band, ch, cells = grad.shape
    return pl.pallas_call(
        input_kernel,
        in_specs=smem(1) + vmem(5),
        out_specs=vmem(1)[0],
        out_shape=jax.ShapeDtypeStruct(grad.shape, BF16),
        scratch_shapes=[
            pltpu.VMEM((3, ch, (band + 2) * cells), BF16),
            pltpu.VMEM((9, ch, ch), BF16),
        ],
        cost_estimate=work(grad, 1),
        compiler_params=pltpu.CompilerParams(vmem_limit_bytes=20 << 20),
        name="input",
    )(core, got, grad, outer, mine, theirs)


def exchange(block):
    return lax.ppermute(block, "core", [(0, 1), (1, 0)])


def across_chips(block):
    pairs = [(i, i + 1) for i in range(1, lax.axis_size(ROWS) - 1, 2)]
    return lax.ppermute(block, ROWS, pairs + [(b, a) for a, b in pairs])


def copies(block, axis):
    return jnp.broadcast_to(block[None], (lax.axis_size(axis), *block.shape))


def swap(parts, axis):
    return lax.all_to_all(parts, axis, 0, 0, tiled=True)


def total(parts):
    return lax.optimization_barrier(parts.astype(F32).sum(0))


def body(features, conv_weight, cotangent, valid_rows):
    band, ch, cells = features.shape
    images = cells // COLS
    near = conv_weight.shape[2]
    half = ch // 2
    core = lax.axis_index("core").astype(jnp.int32)
    limits = lax.dynamic_slice_in_dim(valid_rows, lax.axis_index(CH) * images, images, 0)
    limits = limits - lax.axis_index(ROWS) * band
    share = lax.dynamic_slice_in_dim(conv_weight, core * half, half, 3).reshape(9, near, half)
    inner = exchange(lax.dynamic_slice_in_dim(features, (1 - core) * (band - 1), 1, 0))
    outer = across_chips(lax.dynamic_slice_in_dim(features, core * (band - 1), 1, 0))
    mine = swap(copies(share, CH), CH)
    mine, inner, outer = lax.optimization_barrier((mine, inner, outer))
    theirs = exchange(mine)
    where = core.reshape(1)
    grad_pre, outer_grad, own, sent = call_grad(
        limits, where, inner, features, outer, mine, theirs, cotangent
    )
    got = exchange(sent)
    other = got[: own.shape[0]]
    plane = swap((own + other.astype(F32)).astype(BF16), CH)
    plane, outer_grad = lax.optimization_barrier((plane, across_chips(outer_grad)))
    input_grad = call_input(where, got, grad_pre, outer_grad, mine, theirs)
    block = total(plane).astype(BF16)
    block = total(swap(copies(block, "z_near"), "z_near")).astype(BF16)
    block = swap(copies(block, "z_far"), "z_far")
    block, input_grad = lax.optimization_barrier((block, input_grad))
    mine = total(block)
    theirs = exchange(mine)
    first = core == 0
    weight_grad = jnp.concatenate(
        [jnp.where(first, mine, theirs), jnp.where(first, theirs, mine)], 2
    ).reshape(3, 3, near, ch)
    return input_grad, weight_grad


def solution(mesh):
    names = ("z_far", "z_near", "core", "ch_0", "ch_1")
    split = Mesh(mesh.devices.reshape(4, 4, 2, 4, 4), names)
    placed = (P(ROWS, None, CH), P(None, None, CH, None), P(ROWS, None, CH), P())
    return jax.shard_map(
        body,
        mesh=split,
        in_specs=placed,
        out_specs=(P(ROWS, None, CH), P(None, None, CH, None)),
        check_vma=False,
    )
```

```python
import jax
import jax.numpy as jnp
from jax import lax
from jax.experimental import pallas as pl
from jax.experimental.pallas import tpu as pltpu
from jax.sharding import Mesh
from jax.sharding import PartitionSpec as P

COLS = 128
CH = ("ch_0", "ch_1")
ROWS = ("z_far", "z_near", "core")
BF16 = jnp.bfloat16
F32 = jnp.float32


def dot(a, b, dims):
    return lax.dot_general(a, b, (dims, ((), ())), preferred_element_type=F32)


def side_shift(tile, across):
    lane = lax.broadcasted_iota(jnp.int32, tile.shape, 1)
    moved = pltpu.roll(tile.astype(F32), -across % COLS, 1)
    edge = COLS - 1 if across > 0 else 0
    return jnp.where(lane == edge, 0.0, moved).astype(tile.dtype)


def fill_shifted(out_ref, row, halves):
    half, cells = halves[0].shape
    for k, source in enumerate(halves):
        rows = slice(k * half, (k + 1) * half)
        out_ref[1, rows, pl.ds(row * cells, cells)] = source
        for image in range(cells // COLS):
            tile = source[:, image * COLS : (image + 1) * COLS]
            for side in (0, 2):
                out_ref[side, rows, pl.ds(row * cells + image * COLS, COLS)] = side_shift(tile, side - 1)


def stage_kernel(feat_hbm, cot_hbm, feat_ref, cot_ref, sems):
    loads = [
        pltpu.make_async_copy(feat_hbm, feat_ref, sems.at[0]),
        pltpu.make_async_copy(cot_hbm, cot_ref, sems.at[1]),
    ]
    for load in loads:
        load.start()
    for load in loads:
        load.wait()


def grad_kernel(limits_ref, core_ref, inner_ref, feat_ref, outer_ref, mine_ref, theirs_ref, cot_ref,
                grad_hbm, edge_ref, own_ref, sent_ref, shifted_ref, flat_ref, grad_ref, sems):
    band, ch, cells = cot_ref.shape
    images = cells // COLS
    half = ch // 2
    core = core_ref[0]
    first = core == 0
    near = pl.ds(pl.multiple_of(core * half, half), half)
    far = pl.ds(pl.multiple_of((1 - core) * half, half), half)
    inner = [inner_ref[0, near], inner_ref[0, far]]
    outer = [outer_ref[0, near], outer_ref[0, far]]
    fill_shifted(shifted_ref, 0, [jnp.where(first, o, i) for o, i in zip(outer, inner)])
    for h in range(band):
        fill_shifted(shifted_ref, h + 1, [feat_ref[h, near], feat_ref[h, far]])
    fill_shifted(shifted_ref, band + 1, [jnp.where(first, i, o) for o, i in zip(outer, inner)])
    for h in range(band):
        summed = None
        for r in range(3):
            for c in range(3):
                t = 3 * r + c
                w = jnp.concatenate(
                    [mine_ref[:, t].reshape(ch, half), theirs_ref[:, t].reshape(ch, half)], 1
                )
                x = shifted_ref[c, :, pl.ds((h + r) * cells, cells)]
                term = dot(w, x, ((1,), (0,)))
                summed = term if summed is None else summed + term
        center = jnp.sum(summed, 0, keepdims=True) / ch
        spread = jnp.sum(summed * summed, 0, keepdims=True) / ch - center * center
        inverse = lax.rsqrt(spread + 1e-06)
        normed = (summed - center) * inverse
        keep = jnp.concatenate(
            [jnp.full((1, COLS), jnp.where(h < limits_ref[n], 1.0, 0.0), F32) for n in range(images)], 1
        )
        masked = cot_ref[h].astype(F32) * keep
        total = jnp.sum(masked, 0, keepdims=True) / ch
        cross = jnp.sum(masked * normed, 0, keepdims=True) / ch
        grad = (inverse * (masked - total - normed * cross)).astype(BF16)
        grad_ref[h] = grad
        flat_ref[:, pl.ds(h * cells, cells)] = grad
    parts, taps, near_ch, _ = own_ref.shape
    saves = [pltpu.make_async_copy(grad_ref.at[h], grad_hbm.at[h], sems.at[h]) for h in range(band)]
    for r in range(3):
        for c in range(3):
            t = 3 * r + c
            if t == 1:
                for save in saves:
                    save.start()
            tap = dot(flat_ref[...], shifted_ref[c, :, pl.ds(r * cells, band * cells)], ((1,), (1,)))
            own_ref[:, t] = tap[:, :half].reshape(parts, near_ch, half)
            sent_ref[:parts, t] = tap[:, half:].astype(BF16).reshape(parts, near_ch, half)
    bottom, top = grad_ref[0], grad_ref[band - 1]
    edge_ref[0] = jnp.where(first, bottom, top)
    inner = jnp.where(first, top, bottom)
    for g in range(images * parts):
        n, p = divmod(g, parts)
        sent_ref[parts + g // taps, g % taps] = inner[
            p * near_ch : (p + 1) * near_ch, n * COLS : (n + 1) * COLS
        ]
    for save in saves:
        save.wait()


def input_kernel(core_ref, got_ref, grad_ref, outer_ref, mine_ref, theirs_ref, out_ref, shifted_ref, wt_ref):
    band, ch, cells = grad_ref.shape
    half = ch // 2
    first = core_ref[0] == 0
    parts, taps = mine_ref.shape[:2]
    groups = [got_ref[parts + g // taps, g % taps] for g in range(parts * (cells // COLS))]
    images = [jnp.concatenate(groups[k : k + parts], 0) for k in range(0, len(groups), parts)]
    inner = jnp.concatenate(images, 1)
    outer = outer_ref[0]
    near = pl.ds(pl.multiple_of(core_ref[0] * half, half), half)
    far = pl.ds(pl.multiple_of((1 - core_ref[0]) * half, half), half)
    fill_shifted(shifted_ref, 0, [jnp.where(first, outer, inner)])
    for h in range(band):
        fill_shifted(shifted_ref, h + 1, [grad_ref[h]])
    fill_shifted(shifted_ref, band + 1, [jnp.where(first, inner, outer)])
    for t in range(9):
        wt_ref[t, :half] = mine_ref[:, t].reshape(ch, half).T
        wt_ref[t, half:] = theirs_ref[:, t].reshape(ch, half).T
    for h in range(band):
        summed = None
        for r in range(3):
            for c in range(3):
                x = shifted_ref[2 - c, :, pl.ds((h + 2 - r) * cells, cells)]
                term = dot(wt_ref[3 * r + c], x, ((1,), (0,)))
                summed = term if summed is None else summed + term
        out_ref[h, near] = summed[:half].astype(BF16)
        out_ref[h, far] = summed[half:].astype(BF16)


def vmem(count):
    return [pl.BlockSpec(memory_space=pltpu.VMEM)] * count


def smem(count):
    return [pl.BlockSpec(memory_space=pltpu.SMEM)] * count


def in_hbm(block):
    return pltpu.with_memory_space_constraint(block, pltpu.HBM)


HBM = pl.BlockSpec(memory_space=pltpu.HBM)


def work(block, convs):
    band, ch, cells = block.shape
    return pl.CostEstimate(
        flops=convs * 18 * ch * ch * band * cells, bytes_accessed=convs << 22, transcendentals=0
    )


def call_stage(features, cotangent):
    return pl.pallas_call(
        stage_kernel,
        in_specs=[HBM] * 2,
        out_specs=vmem(2),
        out_shape=[jax.ShapeDtypeStruct(v.shape, v.dtype) for v in (features, cotangent)],
        scratch_shapes=[pltpu.SemaphoreType.DMA((2,))],
        cost_estimate=pl.CostEstimate(flops=1 << 20, bytes_accessed=4 << 20, transcendentals=0),
        compiler_params=pltpu.CompilerParams(vmem_limit_bytes=8 << 20),
        name="stage",
    )(in_hbm(features), in_hbm(cotangent))


def call_grad(limits, core, inner, features, outer, mine, theirs, cotangent):
    band, ch, cells = features.shape
    parts, taps, _, _ = mine.shape
    edge_parts = pl.cdiv(parts * (cells // COLS), taps)
    return pl.pallas_call(
        grad_kernel,
        in_specs=smem(2) + vmem(6),
        out_specs=[HBM] + vmem(3),
        out_shape=[
            pltpu.HBM(features.shape, BF16),
            jax.ShapeDtypeStruct(outer.shape, BF16),
            jax.ShapeDtypeStruct(mine.shape, F32),
            jax.ShapeDtypeStruct((parts + edge_parts, *mine.shape[1:]), BF16),
        ],
        scratch_shapes=[
            pltpu.VMEM((3, ch, (band + 2) * cells), BF16),
            pltpu.VMEM((ch, band * cells), BF16),
            pltpu.VMEM(features.shape, BF16),
            pltpu.SemaphoreType.DMA((band,)),
        ],
        cost_estimate=work(features, 2),
        compiler_params=pltpu.CompilerParams(vmem_limit_bytes=24 << 20),
        name="grad",
    )(limits, core, inner, features, outer, mine, theirs, cotangent)


def call_input(core, got, grad, outer, mine, theirs):
    band, ch, cells = grad.shape
    return pl.pallas_call(
        input_kernel,
        in_specs=smem(1) + vmem(5),
        out_specs=vmem(1)[0],
        out_shape=jax.ShapeDtypeStruct(grad.shape, BF16),
        scratch_shapes=[
            pltpu.VMEM((3, ch, (band + 2) * cells), BF16),
            pltpu.VMEM((9, ch, ch), BF16),
        ],
        cost_estimate=work(grad, 1),
        compiler_params=pltpu.CompilerParams(vmem_limit_bytes=20 << 20),
        name="input",
    )(core, got, grad, outer, mine, theirs)


def exchange(block):
    return lax.ppermute(block, "core", [(0, 1), (1, 0)])


def across_chips(block):
    pairs = [(i, i + 1) for i in range(1, lax.axis_size(ROWS) - 1, 2)]
    return lax.ppermute(block, ROWS, pairs + [(b, a) for a, b in pairs])


def copies(block, axis):
    return jnp.broadcast_to(block[None], (lax.axis_size(axis), *block.shape))


def swap(parts, axis):
    return lax.all_to_all(parts, axis, 0, 0, tiled=True)


def total(parts):
    return lax.optimization_barrier(parts.astype(F32).sum(0))


def body(features, conv_weight, cotangent, valid_rows):
    band, ch, cells = features.shape
    images = cells // COLS
    near = conv_weight.shape[2]
    half = ch // 2
    core = lax.axis_index("core").astype(jnp.int32)
    limits = lax.dynamic_slice_in_dim(valid_rows, lax.axis_index(CH) * images, images, 0)
    limits = limits - lax.axis_index(ROWS) * band
    share = lax.dynamic_slice_in_dim(conv_weight, core * half, half, 3).reshape(9, near, half)
    inner = exchange(lax.dynamic_slice_in_dim(features, (1 - core) * (band - 1), 1, 0))
    outer = across_chips(lax.dynamic_slice_in_dim(features, core * (band - 1), 1, 0))
    mine = swap(copies(share, CH), CH)
    theirs = exchange(mine)
    features, cotangent = call_stage(features, cotangent)
    where = core.reshape(1)
    grad_pre, outer_grad, own, sent = call_grad(
        limits, where, inner, features, outer, mine, theirs, cotangent
    )
    got = exchange(sent)
    other = got[: own.shape[0]]
    plane = swap((own + other.astype(F32)).astype(BF16), CH)
    plane, outer_grad = lax.optimization_barrier((plane, across_chips(outer_grad)))
    input_grad = call_input(where, got, grad_pre, outer_grad, mine, theirs)
    block = total(plane).astype(BF16)
    block = total(swap(copies(block, "z_near"), "z_near")).astype(BF16)
    block = swap(copies(block, "z_far"), "z_far")
    block, input_grad = lax.optimization_barrier((block, input_grad))
    mine = total(block)
    theirs = exchange(mine)
    first = core == 0
    weight_grad = jnp.concatenate(
        [jnp.where(first, mine, theirs), jnp.where(first, theirs, mine)], 2
    ).reshape(3, 3, near, ch)
    return input_grad, weight_grad


def solution(mesh):
    names = ("z_far", "z_near", "core", "ch_0", "ch_1")
    split = Mesh(mesh.devices.reshape(4, 4, 2, 4, 4), names)
    placed = (P(ROWS, None, CH), P(None, None, CH, None), P(ROWS, None, CH), P())
    return jax.shard_map(
        body,
        mesh=split,
        in_specs=placed,
        out_specs=(P(ROWS, None, CH), P(None, None, CH, None)),
        check_vma=False,
    )
```

```python
import jax
import jax.numpy as jnp
from jax import lax
from jax.experimental import pallas as pl
from jax.experimental.pallas import tpu as pltpu
from jax.sharding import Mesh
from jax.sharding import PartitionSpec as P

COLS = 128
CH = ("ch_0", "ch_1")
ROWS = ("z_far", "z_near", "core")
BF16 = jnp.bfloat16
F32 = jnp.float32


def dot(a, b, dims):
    return lax.dot_general(a, b, (dims, ((), ())), preferred_element_type=F32)


def side_shift(tile, across):
    lane = lax.broadcasted_iota(jnp.int32, tile.shape, 1)
    moved = pltpu.roll(tile.astype(F32), -across % COLS, 1)
    edge = COLS - 1 if across > 0 else 0
    return jnp.where(lane == edge, 0.0, moved).astype(tile.dtype)


def fill_shifted(out_ref, row, halves):
    half, cells = halves[0].shape
    for k, source in enumerate(halves):
        rows = slice(k * half, (k + 1) * half)
        out_ref[1, rows, pl.ds(row * cells, cells)] = source
        for image in range(cells // COLS):
            tile = source[:, image * COLS : (image + 1) * COLS]
            for side in (0, 2):
                out_ref[side, rows, pl.ds(row * cells + image * COLS, COLS)] = side_shift(tile, side - 1)


def stage_kernel(feat_hbm, cot_hbm, feat_ref, cot_ref, sems):
    loads = [
        pltpu.make_async_copy(feat_hbm, feat_ref, sems.at[0]),
        pltpu.make_async_copy(cot_hbm, cot_ref, sems.at[1]),
    ]
    for load in loads:
        load.start()
    for load in loads:
        load.wait()


def grad_kernel(limits_ref, core_ref, inner_ref, feat_ref, outer_ref, mine_ref, theirs_ref, cot_ref,
                grad_hbm, edge_ref, own_ref, sent_ref, shifted_ref, flat_ref, grad_ref, sems):
    band, ch, cells = cot_ref.shape
    images = cells // COLS
    half = ch // 2
    core = core_ref[0]
    first = core == 0
    near = pl.ds(pl.multiple_of(core * half, half), half)
    far = pl.ds(pl.multiple_of((1 - core) * half, half), half)
    inner = [inner_ref[0, near], inner_ref[0, far]]
    outer = [outer_ref[0, near], outer_ref[0, far]]
    fill_shifted(shifted_ref, 0, [jnp.where(first, o, i) for o, i in zip(outer, inner)])
    for h in range(band):
        fill_shifted(shifted_ref, h + 1, [feat_ref[h, near], feat_ref[h, far]])
    fill_shifted(shifted_ref, band + 1, [jnp.where(first, i, o) for o, i in zip(outer, inner)])
    for h in range(band):
        summed = None
        for r in range(3):
            for c in range(3):
                t = 3 * r + c
                w = jnp.concatenate(
                    [mine_ref[:, t].reshape(ch, half), theirs_ref[:, t].reshape(ch, half)], 1
                )
                x = shifted_ref[c, :, pl.ds((h + r) * cells, cells)]
                term = dot(w, x, ((1,), (0,)))
                summed = term if summed is None else summed + term
        center = jnp.sum(summed, 0, keepdims=True) / ch
        spread = jnp.sum(summed * summed, 0, keepdims=True) / ch - center * center
        inverse = lax.rsqrt(spread + 1e-06)
        normed = (summed - center) * inverse
        keep = jnp.concatenate(
            [jnp.full((1, COLS), jnp.where(h < limits_ref[n], 1.0, 0.0), F32) for n in range(images)], 1
        )
        masked = cot_ref[h].astype(F32) * keep
        total = jnp.sum(masked, 0, keepdims=True) / ch
        cross = jnp.sum(masked * normed, 0, keepdims=True) / ch
        grad = (inverse * (masked - total - normed * cross)).astype(BF16)
        grad_ref[h] = grad
        flat_ref[:, pl.ds(h * cells, cells)] = grad
    parts, taps, near_ch, _ = own_ref.shape
    saves = [pltpu.make_async_copy(grad_ref.at[h], grad_hbm.at[h], sems.at[h]) for h in range(band)]
    for r in range(3):
        for c in range(3):
            t = 3 * r + c
            if t == 1:
                for save in saves:
                    save.start()
            tap = dot(flat_ref[...], shifted_ref[c, :, pl.ds(r * cells, band * cells)], ((1,), (1,)))
            own_ref[:, t] = tap[:, :half].reshape(parts, near_ch, half)
            sent_ref[:parts, t] = tap[:, half:].astype(BF16).reshape(parts, near_ch, half)
    bottom, top = grad_ref[0], grad_ref[band - 1]
    edge_ref[0] = jnp.where(first, bottom, top)
    inner = jnp.where(first, top, bottom)
    for g in range(images * parts):
        n, p = divmod(g, parts)
        sent_ref[parts + g // taps, g % taps] = inner[
            p * near_ch : (p + 1) * near_ch, n * COLS : (n + 1) * COLS
        ]
    for save in saves:
        save.wait()


def input_kernel(core_ref, got_ref, grad_hbm, outer_ref, mine_ref, theirs_ref, out_ref,
                 grad_ref, shifted_ref, wt_ref, sem):
    band, ch, cells = grad_ref.shape
    half = ch // 2
    load = pltpu.make_async_copy(grad_hbm, grad_ref, sem.at[0])
    load.start()
    for t in range(9):
        wt_ref[t, :half] = mine_ref[:, t].reshape(ch, half).T
        wt_ref[t, half:] = theirs_ref[:, t].reshape(ch, half).T
    first = core_ref[0] == 0
    parts, taps = mine_ref.shape[:2]
    groups = [got_ref[parts + g // taps, g % taps] for g in range(parts * (cells // COLS))]
    images = [jnp.concatenate(groups[k : k + parts], 0) for k in range(0, len(groups), parts)]
    inner = jnp.concatenate(images, 1)
    outer = outer_ref[0]
    near = pl.ds(pl.multiple_of(core_ref[0] * half, half), half)
    far = pl.ds(pl.multiple_of((1 - core_ref[0]) * half, half), half)
    fill_shifted(shifted_ref, 0, [jnp.where(first, outer, inner)])
    fill_shifted(shifted_ref, band + 1, [jnp.where(first, inner, outer)])
    load.wait()
    for h in range(band):
        fill_shifted(shifted_ref, h + 1, [grad_ref[h]])
    for h in range(band):
        summed = None
        for r in range(3):
            for c in range(3):
                x = shifted_ref[2 - c, :, pl.ds((h + 2 - r) * cells, cells)]
                term = dot(wt_ref[3 * r + c], x, ((1,), (0,)))
                summed = term if summed is None else summed + term
        out_ref[h, near] = summed[:half].astype(BF16)
        out_ref[h, far] = summed[half:].astype(BF16)


def vmem(count):
    return [pl.BlockSpec(memory_space=pltpu.VMEM)] * count


def smem(count):
    return [pl.BlockSpec(memory_space=pltpu.SMEM)] * count


def in_hbm(block):
    return pltpu.with_memory_space_constraint(block, pltpu.HBM)


HBM = pl.BlockSpec(memory_space=pltpu.HBM)


def work(block, convs):
    band, ch, cells = block.shape
    return pl.CostEstimate(
        flops=convs * 18 * ch * ch * band * cells, bytes_accessed=convs << 22, transcendentals=0
    )


def call_stage(features, cotangent):
    return pl.pallas_call(
        stage_kernel,
        in_specs=[HBM] * 2,
        out_specs=vmem(2),
        out_shape=[jax.ShapeDtypeStruct(v.shape, v.dtype) for v in (features, cotangent)],
        scratch_shapes=[pltpu.SemaphoreType.DMA((2,))],
        cost_estimate=pl.CostEstimate(flops=1 << 20, bytes_accessed=4 << 20, transcendentals=0),
        compiler_params=pltpu.CompilerParams(vmem_limit_bytes=8 << 20),
        name="stage",
    )(in_hbm(features), in_hbm(cotangent))


def call_grad(limits, core, inner, features, outer, mine, theirs, cotangent):
    band, ch, cells = features.shape
    parts, taps, _, _ = mine.shape
    edge_parts = pl.cdiv(parts * (cells // COLS), taps)
    return pl.pallas_call(
        grad_kernel,
        in_specs=smem(2) + vmem(6),
        out_specs=[HBM] + vmem(3),
        out_shape=[
            pltpu.HBM(features.shape, BF16),
            jax.ShapeDtypeStruct(outer.shape, BF16),
            jax.ShapeDtypeStruct(mine.shape, F32),
            jax.ShapeDtypeStruct((parts + edge_parts, *mine.shape[1:]), BF16),
        ],
        scratch_shapes=[
            pltpu.VMEM((3, ch, (band + 2) * cells), BF16),
            pltpu.VMEM((ch, band * cells), BF16),
            pltpu.VMEM(features.shape, BF16),
            pltpu.SemaphoreType.DMA((band,)),
        ],
        cost_estimate=work(features, 2),
        compiler_params=pltpu.CompilerParams(vmem_limit_bytes=24 << 20),
        name="grad",
    )(limits, core, inner, features, outer, mine, theirs, cotangent)


def call_input(core, got, grad, outer, mine, theirs):
    band, ch, cells = grad.shape
    return pl.pallas_call(
        input_kernel,
        in_specs=smem(1) + vmem(1) + [HBM] + vmem(3),
        out_specs=vmem(1)[0],
        out_shape=jax.ShapeDtypeStruct(grad.shape, BF16),
        scratch_shapes=[
            pltpu.VMEM(grad.shape, BF16),
            pltpu.VMEM((3, ch, (band + 2) * cells), BF16),
            pltpu.VMEM((9, ch, ch), BF16),
            pltpu.SemaphoreType.DMA((1,)),
        ],
        cost_estimate=work(grad, 1),
        compiler_params=pltpu.CompilerParams(vmem_limit_bytes=20 << 20),
        name="input",
    )(core, got, in_hbm(grad), outer, mine, theirs)


def exchange(block):
    return lax.ppermute(block, "core", [(0, 1), (1, 0)])


def across_chips(block):
    pairs = [(i, i + 1) for i in range(1, lax.axis_size(ROWS) - 1, 2)]
    return lax.ppermute(block, ROWS, pairs + [(b, a) for a, b in pairs])


def copies(block, axis):
    return jnp.broadcast_to(block[None], (lax.axis_size(axis), *block.shape))


def swap(parts, axis):
    return lax.all_to_all(parts, axis, 0, 0, tiled=True)


def total(parts):
    return lax.optimization_barrier(parts.astype(F32).sum(0))


def body(features, conv_weight, cotangent, valid_rows):
    band, ch, cells = features.shape
    images = cells // COLS
    near = conv_weight.shape[2]
    half = ch // 2
    core = lax.axis_index("core").astype(jnp.int32)
    limits = lax.dynamic_slice_in_dim(valid_rows, lax.axis_index(CH) * images, images, 0)
    limits = limits - lax.axis_index(ROWS) * band
    share = lax.dynamic_slice_in_dim(conv_weight, core * half, half, 3).reshape(9, near, half)
    inner = exchange(lax.dynamic_slice_in_dim(features, (1 - core) * (band - 1), 1, 0))
    outer = across_chips(lax.dynamic_slice_in_dim(features, core * (band - 1), 1, 0))
    mine = swap(copies(share, CH), CH)
    theirs = exchange(mine)
    features, cotangent = call_stage(features, cotangent)
    where = core.reshape(1)
    grad_pre, outer_grad, own, sent = call_grad(
        limits, where, inner, features, outer, mine, theirs, cotangent
    )
    got = exchange(sent)
    outer_grad = across_chips(outer_grad)
    input_grad = call_input(where, got, grad_pre, outer_grad, mine, theirs)
    other = got[: own.shape[0]]
    pair = (own + other.astype(F32)).astype(BF16)
    plane = swap(pair, CH)
    block = total(plane).astype(BF16)
    block = total(swap(copies(block, "z_near"), "z_near")).astype(BF16)
    block = swap(copies(block, "z_far"), "z_far")
    mine = total(block)
    theirs = exchange(mine)
    first = core == 0
    weight_grad = jnp.concatenate(
        [jnp.where(first, mine, theirs), jnp.where(first, theirs, mine)], 2
    ).reshape(3, 3, near, ch)
    return input_grad, weight_grad


def solution(mesh):
    names = ("z_far", "z_near", "core", "ch_0", "ch_1")
    split = Mesh(mesh.devices.reshape(4, 4, 2, 4, 4), names)
    placed = (P(ROWS, None, CH), P(None, None, CH, None), P(ROWS, None, CH), P())
    return jax.shard_map(
        body,
        mesh=split,
        in_specs=placed,
        out_specs=(P(ROWS, None, CH), P(None, None, CH, None)),
        check_vma=False,
    )
```

```python
import jax
import jax.numpy as jnp
from jax import lax
from jax.experimental import pallas as pl
from jax.experimental.pallas import tpu as pltpu
from jax.sharding import Mesh
from jax.sharding import PartitionSpec as P

COLS = 128
CH = ("ch_0", "ch_1")
ROWS = ("z_far", "z_near", "core")
BF16 = jnp.bfloat16
F32 = jnp.float32


def dot(a, b, dims):
    return lax.dot_general(a, b, (dims, ((), ())), preferred_element_type=F32)


def side_shift(tile, across):
    lane = lax.broadcasted_iota(jnp.int32, tile.shape, 1)
    moved = pltpu.roll(tile.astype(F32), -across % COLS, 1)
    edge = COLS - 1 if across > 0 else 0
    return jnp.where(lane == edge, 0.0, moved).astype(tile.dtype)


def fill_shifted(out_ref, row, halves):
    half, cells = halves[0].shape
    for k, source in enumerate(halves):
        rows = slice(k * half, (k + 1) * half)
        out_ref[1, rows, pl.ds(row * cells, cells)] = source
        for image in range(cells // COLS):
            tile = source[:, image * COLS : (image + 1) * COLS]
            for side in (0, 2):
                out_ref[side, rows, pl.ds(row * cells + image * COLS, COLS)] = side_shift(tile, side - 1)


def stage_kernel(feat_hbm, cot_hbm, feat_ref, cot_ref, sems):
    loads = [
        pltpu.make_async_copy(feat_hbm, feat_ref, sems.at[0]),
        pltpu.make_async_copy(cot_hbm, cot_ref, sems.at[1]),
    ]
    for load in loads:
        load.start()
    for load in loads:
        load.wait()


def grad_kernel(limits_ref, core_ref, inner_ref, feat_ref, outer_ref, mine_ref, theirs_ref, cot_ref,
                grad_hbm, edge_ref, own_ref, sent_ref, shifted_ref, flat_ref, grad_ref, sems):
    band, ch, cells = cot_ref.shape
    images = cells // COLS
    half = ch // 2
    core = core_ref[0]
    first = core == 0
    near = pl.ds(pl.multiple_of(core * half, half), half)
    far = pl.ds(pl.multiple_of((1 - core) * half, half), half)
    inner = [inner_ref[0, near], inner_ref[0, far]]
    outer = [outer_ref[0, near], outer_ref[0, far]]
    fill_shifted(shifted_ref, 0, [jnp.where(first, o, i) for o, i in zip(outer, inner)])
    for h in range(band):
        fill_shifted(shifted_ref, h + 1, [feat_ref[h, near], feat_ref[h, far]])
    fill_shifted(shifted_ref, band + 1, [jnp.where(first, i, o) for o, i in zip(outer, inner)])
    for h in range(band):
        summed = None
        for r in range(3):
            for c in range(3):
                t = 3 * r + c
                w = jnp.concatenate(
                    [mine_ref[:, t].reshape(ch, half), theirs_ref[:, t].reshape(ch, half)], 1
                )
                x = shifted_ref[c, :, pl.ds((h + r) * cells, cells)]
                term = dot(w, x, ((1,), (0,)))
                summed = term if summed is None else summed + term
        center = jnp.sum(summed, 0, keepdims=True) / ch
        spread = jnp.sum(summed * summed, 0, keepdims=True) / ch - center * center
        inverse = lax.rsqrt(spread + 1e-06)
        normed = (summed - center) * inverse
        keep = jnp.concatenate(
            [jnp.full((1, COLS), jnp.where(h < limits_ref[n], 1.0, 0.0), F32) for n in range(images)], 1
        )
        masked = cot_ref[h].astype(F32) * keep
        total = jnp.sum(masked, 0, keepdims=True) / ch
        cross = jnp.sum(masked * normed, 0, keepdims=True) / ch
        grad = (inverse * (masked - total - normed * cross)).astype(BF16)
        grad_ref[h] = grad
        flat_ref[:, pl.ds(h * cells, cells)] = grad
    parts, taps, near_ch, _ = own_ref.shape
    saves = [pltpu.make_async_copy(grad_ref.at[h], grad_hbm.at[h], sems.at[h]) for h in range(band)]
    for r in range(3):
        for c in range(3):
            t = 3 * r + c
            if t == 1:
                for save in saves:
                    save.start()
            tap = dot(flat_ref[...], shifted_ref[c, :, pl.ds(r * cells, band * cells)], ((1,), (1,)))
            own_ref[:, t] = tap[:, :half].reshape(parts, near_ch, half)
            sent_ref[:parts, t] = tap[:, half:].astype(BF16).reshape(parts, near_ch, half)
    bottom, top = grad_ref[0], grad_ref[band - 1]
    edge_ref[0] = jnp.where(first, bottom, top)
    inner = jnp.where(first, top, bottom)
    for g in range(images * parts):
        n, p = divmod(g, parts)
        sent_ref[parts + g // taps, g % taps] = inner[
            p * near_ch : (p + 1) * near_ch, n * COLS : (n + 1) * COLS
        ]
    for save in saves:
        save.wait()


def input_kernel(core_ref, got_ref, grad_ref, outer_ref, mine_ref, theirs_ref, out_ref, shifted_ref, wt_ref):
    band, ch, cells = grad_ref.shape
    half = ch // 2
    first = core_ref[0] == 0
    parts, taps = mine_ref.shape[:2]
    groups = [got_ref[parts + g // taps, g % taps] for g in range(parts * (cells // COLS))]
    images = [jnp.concatenate(groups[k : k + parts], 0) for k in range(0, len(groups), parts)]
    inner = jnp.concatenate(images, 1)
    outer = outer_ref[0]
    near = pl.ds(pl.multiple_of(core_ref[0] * half, half), half)
    far = pl.ds(pl.multiple_of((1 - core_ref[0]) * half, half), half)
    fill_shifted(shifted_ref, 0, [jnp.where(first, outer, inner)])
    for h in range(band):
        fill_shifted(shifted_ref, h + 1, [grad_ref[h]])
    fill_shifted(shifted_ref, band + 1, [jnp.where(first, inner, outer)])
    for t in range(9):
        wt_ref[t, :half] = mine_ref[:, t].reshape(ch, half).T
        wt_ref[t, half:] = theirs_ref[:, t].reshape(ch, half).T
    for h in range(band):
        summed = None
        for r in range(3):
            for c in range(3):
                x = shifted_ref[2 - c, :, pl.ds((h + 2 - r) * cells, cells)]
                term = dot(wt_ref[3 * r + c], x, ((1,), (0,)))
                summed = term if summed is None else summed + term
        out_ref[h, near] = summed[:half].astype(BF16)
        out_ref[h, far] = summed[half:].astype(BF16)


def vmem(count):
    return [pl.BlockSpec(memory_space=pltpu.VMEM)] * count


def smem(count):
    return [pl.BlockSpec(memory_space=pltpu.SMEM)] * count


def in_hbm(block):
    return pltpu.with_memory_space_constraint(block, pltpu.HBM)


HBM = pl.BlockSpec(memory_space=pltpu.HBM)


def work(block, convs):
    band, ch, cells = block.shape
    return pl.CostEstimate(
        flops=convs * 18 * ch * ch * band * cells, bytes_accessed=convs << 22, transcendentals=0
    )


def call_stage(features, cotangent):
    return pl.pallas_call(
        stage_kernel,
        in_specs=[HBM] * 2,
        out_specs=vmem(2),
        out_shape=[jax.ShapeDtypeStruct(v.shape, v.dtype) for v in (features, cotangent)],
        scratch_shapes=[pltpu.SemaphoreType.DMA((2,))],
        cost_estimate=pl.CostEstimate(flops=1 << 20, bytes_accessed=4 << 20, transcendentals=0),
        compiler_params=pltpu.CompilerParams(vmem_limit_bytes=8 << 20),
        name="stage",
    )(in_hbm(features), in_hbm(cotangent))


def call_grad(limits, core, inner, features, outer, mine, theirs, cotangent):
    band, ch, cells = features.shape
    parts, taps, _, _ = mine.shape
    edge_parts = pl.cdiv(parts * (cells // COLS), taps)
    return pl.pallas_call(
        grad_kernel,
        in_specs=smem(2) + vmem(6),
        out_specs=[HBM] + vmem(3),
        out_shape=[
            pltpu.HBM(features.shape, BF16),
            jax.ShapeDtypeStruct(outer.shape, BF16),
            jax.ShapeDtypeStruct(mine.shape, F32),
            jax.ShapeDtypeStruct((parts + edge_parts, *mine.shape[1:]), BF16),
        ],
        scratch_shapes=[
            pltpu.VMEM((3, ch, (band + 2) * cells), BF16),
            pltpu.VMEM((ch, band * cells), BF16),
            pltpu.VMEM(features.shape, BF16),
            pltpu.SemaphoreType.DMA((band,)),
        ],
        cost_estimate=work(features, 2),
        compiler_params=pltpu.CompilerParams(vmem_limit_bytes=24 << 20),
        name="grad",
    )(limits, core, inner, features, outer, mine, theirs, cotangent)


def call_input(core, got, grad, outer, mine, theirs):
    band, ch, cells = grad.shape
    return pl.pallas_call(
        input_kernel,
        in_specs=smem(1) + vmem(5),
        out_specs=vmem(1)[0],
        out_shape=jax.ShapeDtypeStruct(grad.shape, BF16),
        scratch_shapes=[
            pltpu.VMEM((3, ch, (band + 2) * cells), BF16),
            pltpu.VMEM((9, ch, ch), BF16),
        ],
        cost_estimate=work(grad, 1),
        compiler_params=pltpu.CompilerParams(vmem_limit_bytes=20 << 20),
        name="input",
    )(core, got, grad, outer, mine, theirs)


def exchange(block):
    return lax.ppermute(block, "core", [(0, 1), (1, 0)])


def across_chips(block):
    pairs = [(i, i + 1) for i in range(1, lax.axis_size(ROWS) - 1, 2)]
    return lax.ppermute(block, ROWS, pairs + [(b, a) for a, b in pairs])


def copies(block, axis):
    return jnp.broadcast_to(block[None], (lax.axis_size(axis), *block.shape))


def swap(parts, axis):
    return lax.all_to_all(parts, axis, 0, 0, tiled=True)


def total(parts):
    return lax.optimization_barrier(parts.astype(F32).sum(0))


def body(features, conv_weight, cotangent, valid_rows):
    band, ch, cells = features.shape
    images = cells // COLS
    near = conv_weight.shape[2]
    half = ch // 2
    core = lax.axis_index("core").astype(jnp.int32)
    limits = lax.dynamic_slice_in_dim(valid_rows, lax.axis_index(CH) * images, images, 0)
    limits = limits - lax.axis_index(ROWS) * band
    share = lax.dynamic_slice_in_dim(conv_weight, core * half, half, 3).reshape(9, near, half)
    inner = exchange(lax.dynamic_slice_in_dim(features, (1 - core) * (band - 1), 1, 0))
    outer = across_chips(lax.dynamic_slice_in_dim(features, core * (band - 1), 1, 0))
    mine = swap(copies(share, CH), CH)
    theirs = exchange(mine)
    features, cotangent = call_stage(features, cotangent)
    where = core.reshape(1)
    grad_pre, outer_grad, own, sent = call_grad(
        limits, where, inner, features, outer, mine, theirs, cotangent
    )
    got = exchange(sent)
    outer_grad = across_chips(outer_grad)
    input_grad = call_input(where, got, grad_pre, outer_grad, mine, theirs)
    other = got[: own.shape[0]]
    block = total(swap((own + other.astype(F32)).astype(BF16), CH)).astype(BF16)
    block = total(swap(copies(block, "z_near"), "z_near")).astype(BF16)
    block = swap(copies(block, "z_far"), "z_far")
    mine = total(block)
    theirs = exchange(mine)
    first = core == 0
    weight_grad = jnp.concatenate(
        [jnp.where(first, mine, theirs), jnp.where(first, theirs, mine)], 2
    ).reshape(3, 3, near, ch)
    return input_grad, weight_grad


def solution(mesh):
    names = ("z_far", "z_near", "core", "ch_0", "ch_1")
    split = Mesh(mesh.devices.reshape(4, 4, 2, 4, 4), names)
    placed = (P(ROWS, None, CH), P(None, None, CH, None), P(ROWS, None, CH), P())
    return jax.shard_map(
        body,
        mesh=split,
        in_specs=placed,
        out_specs=(P(ROWS, None, CH), P(None, None, CH, None)),
        check_vma=False,
    )
```

```python
import jax
import jax.numpy as jnp
from jax import lax
from jax.experimental import pallas as pl
from jax.experimental.pallas import tpu as pltpu
from jax.sharding import Mesh
from jax.sharding import PartitionSpec as P

COLS = 128
CH = ("ch_0", "ch_1")
ROWS = ("z_far", "z_near", "core")
BF16 = jnp.bfloat16
F32 = jnp.float32


def dot(a, b, dims):
    return lax.dot_general(a, b, (dims, ((), ())), preferred_element_type=F32)


def side_shift(tile, across):
    lane = lax.broadcasted_iota(jnp.int32, tile.shape, 1)
    moved = pltpu.roll(tile.astype(F32), -across % COLS, 1)
    edge = COLS - 1 if across > 0 else 0
    return jnp.where(lane == edge, 0.0, moved).astype(tile.dtype)


def fill_shifted(out_ref, row, halves):
    half, cells = halves[0].shape
    for k, source in enumerate(halves):
        rows = slice(k * half, (k + 1) * half)
        out_ref[1, rows, pl.ds(row * cells, cells)] = source
        for image in range(cells // COLS):
            tile = source[:, image * COLS : (image + 1) * COLS]
            for side in (0, 2):
                out_ref[side, rows, pl.ds(row * cells + image * COLS, COLS)] = side_shift(tile, side - 1)


def stage_kernel(feat_hbm, cot_hbm, feat_ref, cot_ref, sems):
    loads = [
        pltpu.make_async_copy(feat_hbm, feat_ref, sems.at[0]),
        pltpu.make_async_copy(cot_hbm, cot_ref, sems.at[1]),
    ]
    for load in loads:
        load.start()
    for load in loads:
        load.wait()


def grad_kernel(limits_ref, core_ref, inner_ref, feat_ref, outer_ref, mine_ref, theirs_ref, cot_ref,
                grad_hbm, edge_ref, own_ref, sent_ref, shifted_ref, flat_ref, grad_ref, sems):
    band, ch, cells = cot_ref.shape
    images = cells // COLS
    half = ch // 2
    core = core_ref[0]
    first = core == 0
    near = pl.ds(pl.multiple_of(core * half, half), half)
    far = pl.ds(pl.multiple_of((1 - core) * half, half), half)
    inner = [inner_ref[0, near], inner_ref[0, far]]
    outer = [outer_ref[0, near], outer_ref[0, far]]
    fill_shifted(shifted_ref, 0, [jnp.where(first, o, i) for o, i in zip(outer, inner)])
    for h in range(band):
        fill_shifted(shifted_ref, h + 1, [feat_ref[h, near], feat_ref[h, far]])
    fill_shifted(shifted_ref, band + 1, [jnp.where(first, i, o) for o, i in zip(outer, inner)])
    for h in range(band):
        summed = None
        for r in range(3):
            for c in range(3):
                t = 3 * r + c
                w = jnp.concatenate(
                    [mine_ref[:, t].reshape(ch, half), theirs_ref[:, t].reshape(ch, half)], 1
                )
                x = shifted_ref[c, :, pl.ds((h + r) * cells, cells)]
                term = dot(w, x, ((1,), (0,)))
                summed = term if summed is None else summed + term
        center = jnp.sum(summed, 0, keepdims=True) / ch
        spread = jnp.sum(summed * summed, 0, keepdims=True) / ch - center * center
        inverse = lax.rsqrt(spread + 1e-06)
        normed = (summed - center) * inverse
        keep = jnp.concatenate(
            [jnp.full((1, COLS), jnp.where(h < limits_ref[n], 1.0, 0.0), F32) for n in range(images)], 1
        )
        masked = cot_ref[h].astype(F32) * keep
        total = jnp.sum(masked, 0, keepdims=True) / ch
        cross = jnp.sum(masked * normed, 0, keepdims=True) / ch
        grad = (inverse * (masked - total - normed * cross)).astype(BF16)
        grad_ref[h] = grad
        flat_ref[:, pl.ds(h * cells, cells)] = grad
    parts, taps, near_ch, _ = own_ref.shape
    saves = [pltpu.make_async_copy(grad_ref.at[h], grad_hbm.at[h], sems.at[h]) for h in range(band)]
    for r in range(3):
        for c in range(3):
            t = 3 * r + c
            if t == 1:
                for save in saves:
                    save.start()
            tap = dot(flat_ref[...], shifted_ref[c, :, pl.ds(r * cells, band * cells)], ((1,), (1,)))
            own_ref[:, t] = tap[:, :half].reshape(parts, near_ch, half)
            sent_ref[:parts, t] = tap[:, half:].astype(BF16).reshape(parts, near_ch, half)
    bottom, top = grad_ref[0], grad_ref[band - 1]
    edge_ref[0] = jnp.where(first, bottom, top)
    inner = jnp.where(first, top, bottom)
    for g in range(images * parts):
        n, p = divmod(g, parts)
        sent_ref[parts + g // taps, g % taps] = inner[
            p * near_ch : (p + 1) * near_ch, n * COLS : (n + 1) * COLS
        ]
    for save in saves:
        save.wait()


def input_kernel(core_ref, got_ref, grad_ref, outer_ref, mine_ref, theirs_ref, out_ref, shifted_ref, wt_ref):
    band, ch, cells = grad_ref.shape
    half = ch // 2
    first = core_ref[0] == 0
    parts, taps = mine_ref.shape[:2]
    groups = [got_ref[g // taps, g % taps] for g in range(parts * (cells // COLS))]
    images = [jnp.concatenate(groups[k : k + parts], 0) for k in range(0, len(groups), parts)]
    inner = jnp.concatenate(images, 1)
    outer = outer_ref[0]
    near = pl.ds(pl.multiple_of(core_ref[0] * half, half), half)
    far = pl.ds(pl.multiple_of((1 - core_ref[0]) * half, half), half)
    fill_shifted(shifted_ref, 0, [jnp.where(first, outer, inner)])
    for h in range(band):
        fill_shifted(shifted_ref, h + 1, [grad_ref[h]])
    fill_shifted(shifted_ref, band + 1, [jnp.where(first, inner, outer)])
    for t in range(9):
        wt_ref[t, :half] = mine_ref[:, t].reshape(ch, half).T
        wt_ref[t, half:] = theirs_ref[:, t].reshape(ch, half).T
    for h in range(band):
        summed = None
        for r in range(3):
            for c in range(3):
                x = shifted_ref[2 - c, :, pl.ds((h + 2 - r) * cells, cells)]
                term = dot(wt_ref[3 * r + c], x, ((1,), (0,)))
                summed = term if summed is None else summed + term
        out_ref[h, near] = summed[:half].astype(BF16)
        out_ref[h, far] = summed[half:].astype(BF16)


def vmem(count):
    return [pl.BlockSpec(memory_space=pltpu.VMEM)] * count


def smem(count):
    return [pl.BlockSpec(memory_space=pltpu.SMEM)] * count


def in_hbm(block):
    return pltpu.with_memory_space_constraint(block, pltpu.HBM)


HBM = pl.BlockSpec(memory_space=pltpu.HBM)


def work(block, convs):
    band, ch, cells = block.shape
    return pl.CostEstimate(
        flops=convs * 18 * ch * ch * band * cells, bytes_accessed=convs << 22, transcendentals=0
    )


def call_stage(features, cotangent):
    return pl.pallas_call(
        stage_kernel,
        in_specs=[HBM] * 2,
        out_specs=vmem(2),
        out_shape=[jax.ShapeDtypeStruct(v.shape, v.dtype) for v in (features, cotangent)],
        scratch_shapes=[pltpu.SemaphoreType.DMA((2,))],
        cost_estimate=pl.CostEstimate(flops=1 << 20, bytes_accessed=4 << 20, transcendentals=0),
        compiler_params=pltpu.CompilerParams(vmem_limit_bytes=8 << 20),
        name="stage",
    )(in_hbm(features), in_hbm(cotangent))


def call_grad(limits, core, inner, features, outer, mine, theirs, cotangent):
    band, ch, cells = features.shape
    parts, taps, _, _ = mine.shape
    edge_parts = pl.cdiv(parts * (cells // COLS), taps)
    return pl.pallas_call(
        grad_kernel,
        in_specs=smem(2) + vmem(6),
        out_specs=[HBM] + vmem(3),
        out_shape=[
            pltpu.HBM(features.shape, BF16),
            jax.ShapeDtypeStruct(outer.shape, BF16),
            jax.ShapeDtypeStruct(mine.shape, F32),
            jax.ShapeDtypeStruct((parts + edge_parts, *mine.shape[1:]), BF16),
        ],
        scratch_shapes=[
            pltpu.VMEM((3, ch, (band + 2) * cells), BF16),
            pltpu.VMEM((ch, band * cells), BF16),
            pltpu.VMEM(features.shape, BF16),
            pltpu.SemaphoreType.DMA((band,)),
        ],
        cost_estimate=work(features, 2),
        compiler_params=pltpu.CompilerParams(vmem_limit_bytes=24 << 20),
        name="grad",
    )(limits, core, inner, features, outer, mine, theirs, cotangent)


def call_input(core, got, grad, outer, mine, theirs):
    band, ch, cells = grad.shape
    return pl.pallas_call(
        input_kernel,
        in_specs=smem(1) + vmem(5),
        out_specs=vmem(1)[0],
        out_shape=jax.ShapeDtypeStruct(grad.shape, BF16),
        scratch_shapes=[
            pltpu.VMEM((3, ch, (band + 2) * cells), BF16),
            pltpu.VMEM((9, ch, ch), BF16),
        ],
        cost_estimate=work(grad, 1),
        compiler_params=pltpu.CompilerParams(vmem_limit_bytes=20 << 20),
        name="input",
    )(core, got, grad, outer, mine, theirs)


def exchange(block):
    return lax.ppermute(block, "core", [(0, 1), (1, 0)])


def across_chips(block):
    pairs = [(i, i + 1) for i in range(1, lax.axis_size(ROWS) - 1, 2)]
    return lax.ppermute(block, ROWS, pairs + [(b, a) for a, b in pairs])


def copies(block, axis):
    return jnp.broadcast_to(block[None], (lax.axis_size(axis), *block.shape))


def swap(parts, axis):
    return lax.all_to_all(parts, axis, 0, 0, tiled=True)


def total(parts):
    return lax.optimization_barrier(parts.astype(F32).sum(0))


def body(features, conv_weight, cotangent, valid_rows):
    band, ch, cells = features.shape
    images = cells // COLS
    near = conv_weight.shape[2]
    half = ch // 2
    core = lax.axis_index("core").astype(jnp.int32)
    limits = lax.dynamic_slice_in_dim(valid_rows, lax.axis_index(CH) * images, images, 0)
    limits = limits - lax.axis_index(ROWS) * band
    share = lax.dynamic_slice_in_dim(conv_weight, core * half, half, 3).reshape(9, near, half)
    inner = exchange(lax.dynamic_slice_in_dim(features, (1 - core) * (band - 1), 1, 0))
    outer = across_chips(lax.dynamic_slice_in_dim(features, core * (band - 1), 1, 0))
    mine = swap(copies(share, CH), CH)
    theirs = exchange(mine)
    features, cotangent = call_stage(features, cotangent)
    where = core.reshape(1)
    grad_pre, outer_grad, own, sent = call_grad(
        limits, where, inner, features, outer, mine, theirs, cotangent
    )
    got = exchange(sent)
    outer_grad = across_chips(outer_grad)
    parts = own.shape[0]
    pair = (own + got[:parts].astype(F32)).astype(BF16)
    pair, inner_grad = lax.optimization_barrier((pair, got[parts:]))
    input_grad = call_input(where, inner_grad, grad_pre, outer_grad, mine, theirs)
    block = total(swap(pair, CH)).astype(BF16)
    block = total(swap(copies(block, "z_near"), "z_near")).astype(BF16)
    block = swap(copies(block, "z_far"), "z_far")
    mine = total(block)
    theirs = exchange(mine)
    first = core == 0
    weight_grad = jnp.concatenate(
        [jnp.where(first, mine, theirs), jnp.where(first, theirs, mine)], 2
    ).reshape(3, 3, near, ch)
    return input_grad, weight_grad


def solution(mesh):
    names = ("z_far", "z_near", "core", "ch_0", "ch_1")
    split = Mesh(mesh.devices.reshape(4, 4, 2, 4, 4), names)
    placed = (P(ROWS, None, CH), P(None, None, CH, None), P(ROWS, None, CH), P())
    return jax.shard_map(
        body,
        mesh=split,
        in_specs=placed,
        out_specs=(P(ROWS, None, CH), P(None, None, CH, None)),
        check_vma=False,
    )
```

```python
import jax
import jax.numpy as jnp
from jax import lax
from jax.experimental import pallas as pl
from jax.experimental.pallas import tpu as pltpu
from jax.sharding import Mesh
from jax.sharding import PartitionSpec as P

COLS = 128
CH = ("ch_0", "ch_1")
ROWS = ("z_far", "z_near", "core")
BF16 = jnp.bfloat16
F32 = jnp.float32


def dot(a, b, dims):
    return lax.dot_general(a, b, (dims, ((), ())), preferred_element_type=F32)


def side_shift(tile, across):
    lane = lax.broadcasted_iota(jnp.int32, tile.shape, 1)
    moved = pltpu.roll(tile.astype(F32), -across % COLS, 1)
    edge = COLS - 1 if across > 0 else 0
    return jnp.where(lane == edge, 0.0, moved).astype(tile.dtype)


def fill_shifted(out_ref, row, halves):
    half, cells = halves[0].shape
    for k, source in enumerate(halves):
        rows = slice(k * half, (k + 1) * half)
        out_ref[1, rows, pl.ds(row * cells, cells)] = source
        for image in range(cells // COLS):
            tile = source[:, image * COLS : (image + 1) * COLS]
            for side in (0, 2):
                out_ref[side, rows, pl.ds(row * cells + image * COLS, COLS)] = side_shift(tile, side - 1)


def spread_kernel(core_ref, weight_hbm, out_hbm, half_ref, sems):
    peers, _, _, half = out_hbm.shape
    lanes = pl.ds(pl.multiple_of(core_ref[0] * half, half), half)
    load = pltpu.make_async_copy(weight_hbm.at[:, :, lanes], half_ref, sems.at[peers])
    load.start()
    load.wait()
    saves = [pltpu.make_async_copy(half_ref, out_hbm.at[p], sems.at[p]) for p in range(peers)]
    for save in saves:
        save.start()
    for save in saves:
        save.wait()


def stage_kernel(feat_hbm, cot_hbm, feat_ref, cot_ref, sems):
    loads = [
        pltpu.make_async_copy(feat_hbm, feat_ref, sems.at[0]),
        pltpu.make_async_copy(cot_hbm, cot_ref, sems.at[1]),
    ]
    for load in loads:
        load.start()
    for load in loads:
        load.wait()


def grad_kernel(limits_ref, core_ref, inner_ref, feat_ref, outer_ref, mine_ref, theirs_ref, cot_ref,
                grad_hbm, edge_ref, own_ref, sent_ref, shifted_ref, flat_ref, grad_ref, sems):
    band, ch, cells = cot_ref.shape
    images = cells // COLS
    half = ch // 2
    core = core_ref[0]
    first = core == 0
    near = pl.ds(pl.multiple_of(core * half, half), half)
    far = pl.ds(pl.multiple_of((1 - core) * half, half), half)
    inner = [inner_ref[0, near], inner_ref[0, far]]
    outer = [outer_ref[0, near], outer_ref[0, far]]
    fill_shifted(shifted_ref, 0, [jnp.where(first, o, i) for o, i in zip(outer, inner)])
    for h in range(band):
        fill_shifted(shifted_ref, h + 1, [feat_ref[h, near], feat_ref[h, far]])
    fill_shifted(shifted_ref, band + 1, [jnp.where(first, i, o) for o, i in zip(outer, inner)])
    for h in range(band):
        summed = None
        for r in range(3):
            for c in range(3):
                t = 3 * r + c
                w = jnp.concatenate(
                    [mine_ref[:, t].reshape(ch, half), theirs_ref[:, t].reshape(ch, half)], 1
                )
                x = shifted_ref[c, :, pl.ds((h + r) * cells, cells)]
                term = dot(w, x, ((1,), (0,)))
                summed = term if summed is None else summed + term
        center = jnp.sum(summed, 0, keepdims=True) / ch
        spread = jnp.sum(summed * summed, 0, keepdims=True) / ch - center * center
        inverse = lax.rsqrt(spread + 1e-06)
        normed = (summed - center) * inverse
        keep = jnp.concatenate(
            [jnp.full((1, COLS), jnp.where(h < limits_ref[n], 1.0, 0.0), F32) for n in range(images)], 1
        )
        masked = cot_ref[h].astype(F32) * keep
        total = jnp.sum(masked, 0, keepdims=True) / ch
        cross = jnp.sum(masked * normed, 0, keepdims=True) / ch
        grad = (inverse * (masked - total - normed * cross)).astype(BF16)
        grad_ref[h] = grad
        flat_ref[:, pl.ds(h * cells, cells)] = grad
    parts, taps, near_ch, _ = own_ref.shape
    saves = [pltpu.make_async_copy(grad_ref.at[h], grad_hbm.at[h], sems.at[h]) for h in range(band)]
    for r in range(3):
        for c in range(3):
            t = 3 * r + c
            if t == 1:
                for save in saves:
                    save.start()
            tap = dot(flat_ref[...], shifted_ref[c, :, pl.ds(r * cells, band * cells)], ((1,), (1,)))
            own_ref[:, t] = tap[:, :half].reshape(parts, near_ch, half)
            sent_ref[:parts, t] = tap[:, half:].astype(BF16).reshape(parts, near_ch, half)
    bottom, top = grad_ref[0], grad_ref[band - 1]
    edge_ref[0] = jnp.where(first, bottom, top)
    inner = jnp.where(first, top, bottom)
    for g in range(images * parts):
        n, p = divmod(g, parts)
        sent_ref[parts + g // taps, g % taps] = inner[
            p * near_ch : (p + 1) * near_ch, n * COLS : (n + 1) * COLS
        ]
    for save in saves:
        save.wait()


def input_kernel(core_ref, got_ref, grad_ref, outer_ref, mine_ref, theirs_ref, out_ref, shifted_ref, wt_ref):
    band, ch, cells = grad_ref.shape
    half = ch // 2
    first = core_ref[0] == 0
    parts, taps = mine_ref.shape[:2]
    groups = [got_ref[g // taps, g % taps] for g in range(parts * (cells // COLS))]
    images = [jnp.concatenate(groups[k : k + parts], 0) for k in range(0, len(groups), parts)]
    inner = jnp.concatenate(images, 1)
    outer = outer_ref[0]
    near = pl.ds(pl.multiple_of(core_ref[0] * half, half), half)
    far = pl.ds(pl.multiple_of((1 - core_ref[0]) * half, half), half)
    fill_shifted(shifted_ref, 0, [jnp.where(first, outer, inner)])
    for h in range(band):
        fill_shifted(shifted_ref, h + 1, [grad_ref[h]])
    fill_shifted(shifted_ref, band + 1, [jnp.where(first, inner, outer)])
    for t in range(9):
        wt_ref[t, :half] = mine_ref[:, t].reshape(ch, half).T
        wt_ref[t, half:] = theirs_ref[:, t].reshape(ch, half).T
    for h in range(band):
        summed = None
        for r in range(3):
            for c in range(3):
                x = shifted_ref[2 - c, :, pl.ds((h + 2 - r) * cells, cells)]
                term = dot(wt_ref[3 * r + c], x, ((1,), (0,)))
                summed = term if summed is None else summed + term
        out_ref[h, near] = summed[:half].astype(BF16)
        out_ref[h, far] = summed[half:].astype(BF16)


def vmem(count):
    return [pl.BlockSpec(memory_space=pltpu.VMEM)] * count


def smem(count):
    return [pl.BlockSpec(memory_space=pltpu.SMEM)] * count


def in_hbm(block):
    return pltpu.with_memory_space_constraint(block, pltpu.HBM)


HBM = pl.BlockSpec(memory_space=pltpu.HBM)


def work(block, convs):
    band, ch, cells = block.shape
    return pl.CostEstimate(
        flops=convs * 18 * ch * ch * band * cells, bytes_accessed=convs << 22, transcendentals=0
    )


def call_spread(core, weight, peers):
    taps, near_ch, ch = weight.shape
    part = (taps, near_ch, ch // 2)
    return pl.pallas_call(
        spread_kernel,
        in_specs=smem(1) + [HBM],
        out_specs=HBM,
        out_shape=pltpu.HBM((peers, *part), BF16),
        scratch_shapes=[pltpu.VMEM(part, BF16), pltpu.SemaphoreType.DMA((peers + 1,))],
        cost_estimate=pl.CostEstimate(flops=1 << 10, bytes_accessed=1 << 20, transcendentals=0),
        compiler_params=pltpu.CompilerParams(vmem_limit_bytes=4 << 20),
        name="spread",
    )(core, in_hbm(weight))


def call_stage(features, cotangent):
    return pl.pallas_call(
        stage_kernel,
        in_specs=[HBM] * 2,
        out_specs=vmem(2),
        out_shape=[jax.ShapeDtypeStruct(v.shape, v.dtype) for v in (features, cotangent)],
        scratch_shapes=[pltpu.SemaphoreType.DMA((2,))],
        cost_estimate=pl.CostEstimate(flops=1 << 20, bytes_accessed=4 << 20, transcendentals=0),
        compiler_params=pltpu.CompilerParams(vmem_limit_bytes=8 << 20),
        name="stage",
    )(in_hbm(features), in_hbm(cotangent))


def call_grad(limits, core, inner, features, outer, mine, theirs, cotangent):
    band, ch, cells = features.shape
    parts, taps, _, _ = mine.shape
    edge_parts = pl.cdiv(parts * (cells // COLS), taps)
    return pl.pallas_call(
        grad_kernel,
        in_specs=smem(2) + vmem(6),
        out_specs=[HBM] + vmem(3),
        out_shape=[
            pltpu.HBM(features.shape, BF16),
            jax.ShapeDtypeStruct(outer.shape, BF16),
            jax.ShapeDtypeStruct(mine.shape, F32),
            jax.ShapeDtypeStruct((parts + edge_parts, *mine.shape[1:]), BF16),
        ],
        scratch_shapes=[
            pltpu.VMEM((3, ch, (band + 2) * cells), BF16),
            pltpu.VMEM((ch, band * cells), BF16),
            pltpu.VMEM(features.shape, BF16),
            pltpu.SemaphoreType.DMA((band,)),
        ],
        cost_estimate=work(features, 2),
        compiler_params=pltpu.CompilerParams(vmem_limit_bytes=24 << 20),
        name="grad",
    )(limits, core, inner, features, outer, mine, theirs, cotangent)


def call_input(core, got, grad, outer, mine, theirs):
    band, ch, cells = grad.shape
    return pl.pallas_call(
        input_kernel,
        in_specs=smem(1) + vmem(5),
        out_specs=vmem(1)[0],
        out_shape=jax.ShapeDtypeStruct(grad.shape, BF16),
        scratch_shapes=[
            pltpu.VMEM((3, ch, (band + 2) * cells), BF16),
            pltpu.VMEM((9, ch, ch), BF16),
        ],
        cost_estimate=work(grad, 1),
        compiler_params=pltpu.CompilerParams(vmem_limit_bytes=20 << 20),
        name="input",
    )(core, got, grad, outer, mine, theirs)


def exchange(block):
    return lax.ppermute(block, "core", [(0, 1), (1, 0)])


def across_chips(block):
    pairs = [(i, i + 1) for i in range(1, lax.axis_size(ROWS) - 1, 2)]
    return lax.ppermute(block, ROWS, pairs + [(b, a) for a, b in pairs])


def copies(block, axis):
    return jnp.broadcast_to(block[None], (lax.axis_size(axis), *block.shape))


def swap(parts, axis):
    return lax.all_to_all(parts, axis, 0, 0, tiled=True)


def total(parts):
    return lax.optimization_barrier(parts.astype(F32).sum(0))


def body(features, conv_weight, cotangent, valid_rows):
    band, ch, cells = features.shape
    images = cells // COLS
    near = conv_weight.shape[2]
    core = lax.axis_index("core").astype(jnp.int32)
    limits = lax.dynamic_slice_in_dim(valid_rows, lax.axis_index(CH) * images, images, 0)
    limits = limits - lax.axis_index(ROWS) * band
    where = core.reshape(1)
    shares = call_spread(where, conv_weight.reshape(9, near, ch), lax.axis_size(CH))
    inner = exchange(lax.dynamic_slice_in_dim(features, (1 - core) * (band - 1), 1, 0))
    outer = across_chips(lax.dynamic_slice_in_dim(features, core * (band - 1), 1, 0))
    mine = swap(shares, CH)
    theirs = exchange(mine)
    features, cotangent = call_stage(features, cotangent)
    grad_pre, outer_grad, own, sent = call_grad(
        limits, where, inner, features, outer, mine, theirs, cotangent
    )
    got = exchange(sent)
    outer_grad = across_chips(outer_grad)
    parts = own.shape[0]
    pair = (own + got[:parts].astype(F32)).astype(BF16)
    pair, inner_grad = lax.optimization_barrier((pair, got[parts:]))
    input_grad = call_input(where, inner_grad, grad_pre, outer_grad, mine, theirs)
    block = total(swap(pair, CH)).astype(BF16)
    block = total(swap(copies(block, "z_near"), "z_near")).astype(BF16)
    block = swap(copies(block, "z_far"), "z_far")
    mine = total(block)
    theirs = exchange(mine)
    first = core == 0
    weight_grad = jnp.concatenate(
        [jnp.where(first, mine, theirs), jnp.where(first, theirs, mine)], 2
    ).reshape(3, 3, near, ch)
    return input_grad, weight_grad


def solution(mesh):
    names = ("z_far", "z_near", "core", "ch_0", "ch_1")
    split = Mesh(mesh.devices.reshape(4, 4, 2, 4, 4), names)
    placed = (P(ROWS, None, CH), P(None, None, CH, None), P(ROWS, None, CH), P())
    return jax.shard_map(
        body,
        mesh=split,
        in_specs=placed,
        out_specs=(P(ROWS, None, CH), P(None, None, CH, None)),
        check_vma=False,
    )
```

```python
import jax
import jax.numpy as jnp
from jax import lax
from jax.experimental import pallas as pl
from jax.experimental.pallas import tpu as pltpu
from jax.sharding import Mesh
from jax.sharding import PartitionSpec as P

COLS = 128
CH = ("ch_0", "ch_1")
ROWS = ("z_far", "z_near", "core")
BF16 = jnp.bfloat16
F32 = jnp.float32


def dot(a, b, dims):
    return lax.dot_general(a, b, (dims, ((), ())), preferred_element_type=F32)


def side_shift(tile, across):
    lane = lax.broadcasted_iota(jnp.int32, tile.shape, 1)
    moved = pltpu.roll(tile.astype(F32), -across % COLS, 1)
    edge = COLS - 1 if across > 0 else 0
    return jnp.where(lane == edge, 0.0, moved).astype(tile.dtype)


def fill_shifted(out_ref, row, halves):
    half, cells = halves[0].shape
    for k, source in enumerate(halves):
        rows = slice(k * half, (k + 1) * half)
        out_ref[1, rows, pl.ds(row * cells, cells)] = source
        for image in range(cells // COLS):
            tile = source[:, image * COLS : (image + 1) * COLS]
            for side in (0, 2):
                out_ref[side, rows, pl.ds(row * cells + image * COLS, COLS)] = side_shift(tile, side - 1)


def spread_kernel(core_ref, weight_hbm, out_hbm, half_ref, sems):
    peers, _, _, half = out_hbm.shape
    lanes = pl.ds(pl.multiple_of(core_ref[0] * half, half), half)
    load = pltpu.make_async_copy(weight_hbm.at[:, :, lanes], half_ref, sems.at[peers])
    load.start()
    load.wait()
    saves = [pltpu.make_async_copy(half_ref, out_hbm.at[p], sems.at[p]) for p in range(peers)]
    for save in saves:
        save.start()
    for save in saves:
        save.wait()


def sum_kernel(parts_ref, out_ref):
    summed = parts_ref[0].astype(F32)
    for p in range(1, parts_ref.shape[0]):
        summed = summed + parts_ref[p].astype(F32)
    for p in range(out_ref.shape[0]):
        out_ref[p] = summed.astype(BF16)


def join_kernel(core_ref, mine_ref, theirs_ref, out_hbm, sems):
    half = mine_ref.shape[2]
    near = pl.ds(pl.multiple_of(core_ref[0] * half, half), half)
    far = pl.ds(pl.multiple_of((1 - core_ref[0]) * half, half), half)
    saves = [
        pltpu.make_async_copy(mine_ref, out_hbm.at[:, :, near], sems.at[0]),
        pltpu.make_async_copy(theirs_ref, out_hbm.at[:, :, far], sems.at[1]),
    ]
    for save in saves:
        save.start()
    for save in saves:
        save.wait()


def stage_kernel(feat_hbm, cot_hbm, feat_ref, cot_ref, sems):
    loads = [
        pltpu.make_async_copy(feat_hbm, feat_ref, sems.at[0]),
        pltpu.make_async_copy(cot_hbm, cot_ref, sems.at[1]),
    ]
    for load in loads:
        load.start()
    for load in loads:
        load.wait()


def grad_kernel(limits_ref, core_ref, inner_ref, feat_ref, outer_ref, mine_ref, theirs_ref, cot_ref,
                grad_hbm, edge_ref, own_ref, sent_ref, shifted_ref, flat_ref, grad_ref, sems):
    band, ch, cells = cot_ref.shape
    images = cells // COLS
    half = ch // 2
    core = core_ref[0]
    first = core == 0
    near = pl.ds(pl.multiple_of(core * half, half), half)
    far = pl.ds(pl.multiple_of((1 - core) * half, half), half)
    inner = [inner_ref[0, near], inner_ref[0, far]]
    outer = [outer_ref[0, near], outer_ref[0, far]]
    fill_shifted(shifted_ref, 0, [jnp.where(first, o, i) for o, i in zip(outer, inner)])
    for h in range(band):
        fill_shifted(shifted_ref, h + 1, [feat_ref[h, near], feat_ref[h, far]])
    fill_shifted(shifted_ref, band + 1, [jnp.where(first, i, o) for o, i in zip(outer, inner)])
    for h in range(band):
        summed = None
        for r in range(3):
            for c in range(3):
                t = 3 * r + c
                w = jnp.concatenate(
                    [mine_ref[:, t].reshape(ch, half), theirs_ref[:, t].reshape(ch, half)], 1
                )
                x = shifted_ref[c, :, pl.ds((h + r) * cells, cells)]
                term = dot(w, x, ((1,), (0,)))
                summed = term if summed is None else summed + term
        center = jnp.sum(summed, 0, keepdims=True) / ch
        spread = jnp.sum(summed * summed, 0, keepdims=True) / ch - center * center
        inverse = lax.rsqrt(spread + 1e-06)
        normed = (summed - center) * inverse
        keep = jnp.concatenate(
            [jnp.full((1, COLS), jnp.where(h < limits_ref[n], 1.0, 0.0), F32) for n in range(images)], 1
        )
        masked = cot_ref[h].astype(F32) * keep
        total = jnp.sum(masked, 0, keepdims=True) / ch
        cross = jnp.sum(masked * normed, 0, keepdims=True) / ch
        grad = (inverse * (masked - total - normed * cross)).astype(BF16)
        grad_ref[h] = grad
        flat_ref[:, pl.ds(h * cells, cells)] = grad
    parts, taps, near_ch, _ = own_ref.shape
    saves = [pltpu.make_async_copy(grad_ref.at[h], grad_hbm.at[h], sems.at[h]) for h in range(band)]
    for r in range(3):
        for c in range(3):
            t = 3 * r + c
            if t == 1:
                for save in saves:
                    save.start()
            tap = dot(flat_ref[...], shifted_ref[c, :, pl.ds(r * cells, band * cells)], ((1,), (1,)))
            own_ref[:, t] = tap[:, :half].reshape(parts, near_ch, half)
            sent_ref[:parts, t] = tap[:, half:].astype(BF16).reshape(parts, near_ch, half)
    bottom, top = grad_ref[0], grad_ref[band - 1]
    edge_ref[0] = jnp.where(first, bottom, top)
    inner = jnp.where(first, top, bottom)
    for g in range(images * parts):
        n, p = divmod(g, parts)
        sent_ref[parts + g // taps, g % taps] = inner[
            p * near_ch : (p + 1) * near_ch, n * COLS : (n + 1) * COLS
        ]
    for save in saves:
        save.wait()


def input_kernel(core_ref, got_ref, grad_ref, outer_ref, mine_ref, theirs_ref, out_ref, shifted_ref, wt_ref):
    band, ch, cells = grad_ref.shape
    half = ch // 2
    first = core_ref[0] == 0
    parts, taps = mine_ref.shape[:2]
    groups = [got_ref[g // taps, g % taps] for g in range(parts * (cells // COLS))]
    images = [jnp.concatenate(groups[k : k + parts], 0) for k in range(0, len(groups), parts)]
    inner = jnp.concatenate(images, 1)
    outer = outer_ref[0]
    near = pl.ds(pl.multiple_of(core_ref[0] * half, half), half)
    far = pl.ds(pl.multiple_of((1 - core_ref[0]) * half, half), half)
    fill_shifted(shifted_ref, 0, [jnp.where(first, outer, inner)])
    for h in range(band):
        fill_shifted(shifted_ref, h + 1, [grad_ref[h]])
    fill_shifted(shifted_ref, band + 1, [jnp.where(first, inner, outer)])
    for t in range(9):
        wt_ref[t, :half] = mine_ref[:, t].reshape(ch, half).T
        wt_ref[t, half:] = theirs_ref[:, t].reshape(ch, half).T
    for h in range(band):
        summed = None
        for r in range(3):
            for c in range(3):
                x = shifted_ref[2 - c, :, pl.ds((h + 2 - r) * cells, cells)]
                term = dot(wt_ref[3 * r + c], x, ((1,), (0,)))
                summed = term if summed is None else summed + term
        out_ref[h, near] = summed[:half].astype(BF16)
        out_ref[h, far] = summed[half:].astype(BF16)


def vmem(count):
    return [pl.BlockSpec(memory_space=pltpu.VMEM)] * count


def smem(count):
    return [pl.BlockSpec(memory_space=pltpu.SMEM)] * count


def in_hbm(block):
    return pltpu.with_memory_space_constraint(block, pltpu.HBM)


HBM = pl.BlockSpec(memory_space=pltpu.HBM)


def work(block, convs):
    band, ch, cells = block.shape
    return pl.CostEstimate(
        flops=convs * 18 * ch * ch * band * cells, bytes_accessed=convs << 22, transcendentals=0
    )


def call_spread(core, weight, peers):
    taps, near_ch, ch = weight.shape
    part = (taps, near_ch, ch // 2)
    return pl.pallas_call(
        spread_kernel,
        in_specs=smem(1) + [HBM],
        out_specs=HBM,
        out_shape=pltpu.HBM((peers, *part), BF16),
        scratch_shapes=[pltpu.VMEM(part, BF16), pltpu.SemaphoreType.DMA((peers + 1,))],
        cost_estimate=pl.CostEstimate(flops=1 << 10, bytes_accessed=1 << 20, transcendentals=0),
        compiler_params=pltpu.CompilerParams(vmem_limit_bytes=4 << 20),
        name="spread",
    )(core, in_hbm(weight))


def call_sum(parts, copies):
    return pl.pallas_call(
        sum_kernel,
        in_specs=vmem(1),
        out_specs=vmem(1)[0],
        out_shape=jax.ShapeDtypeStruct((copies, *parts.shape[1:]), BF16),
        cost_estimate=pl.CostEstimate(flops=1 << 18, bytes_accessed=1 << 18, transcendentals=0),
        compiler_params=pltpu.CompilerParams(vmem_limit_bytes=4 << 20),
        name="sum",
    )(parts)


def call_join(core, mine, theirs):
    taps, near_ch, half = mine.shape
    return pl.pallas_call(
        join_kernel,
        in_specs=smem(1) + vmem(2),
        out_specs=HBM,
        out_shape=pltpu.HBM((taps, near_ch, 2 * half), F32),
        scratch_shapes=[pltpu.SemaphoreType.DMA((2,))],
        cost_estimate=pl.CostEstimate(flops=1 << 10, bytes_accessed=1 << 18, transcendentals=0),
        compiler_params=pltpu.CompilerParams(vmem_limit_bytes=4 << 20),
        name="join",
    )(core, mine, theirs)


def call_stage(features, cotangent):
    return pl.pallas_call(
        stage_kernel,
        in_specs=[HBM] * 2,
        out_specs=vmem(2),
        out_shape=[jax.ShapeDtypeStruct(v.shape, v.dtype) for v in (features, cotangent)],
        scratch_shapes=[pltpu.SemaphoreType.DMA((2,))],
        cost_estimate=pl.CostEstimate(flops=1 << 20, bytes_accessed=4 << 20, transcendentals=0),
        compiler_params=pltpu.CompilerParams(vmem_limit_bytes=8 << 20),
        name="stage",
    )(in_hbm(features), in_hbm(cotangent))


def call_grad(limits, core, inner, features, outer, mine, theirs, cotangent):
    band, ch, cells = features.shape
    parts, taps, _, _ = mine.shape
    edge_parts = pl.cdiv(parts * (cells // COLS), taps)
    return pl.pallas_call(
        grad_kernel,
        in_specs=smem(2) + vmem(6),
        out_specs=[HBM] + vmem(3),
        out_shape=[
            pltpu.HBM(features.shape, BF16),
            jax.ShapeDtypeStruct(outer.shape, BF16),
            jax.ShapeDtypeStruct(mine.shape, F32),
            jax.ShapeDtypeStruct((parts + edge_parts, *mine.shape[1:]), BF16),
        ],
        scratch_shapes=[
            pltpu.VMEM((3, ch, (band + 2) * cells), BF16),
            pltpu.VMEM((ch, band * cells), BF16),
            pltpu.VMEM(features.shape, BF16),
            pltpu.SemaphoreType.DMA((band,)),
        ],
        cost_estimate=work(features, 2),
        compiler_params=pltpu.CompilerParams(vmem_limit_bytes=24 << 20),
        name="grad",
    )(limits, core, inner, features, outer, mine, theirs, cotangent)


def call_input(core, got, grad, outer, mine, theirs):
    band, ch, cells = grad.shape
    return pl.pallas_call(
        input_kernel,
        in_specs=smem(1) + vmem(5),
        out_specs=vmem(1)[0],
        out_shape=jax.ShapeDtypeStruct(grad.shape, BF16),
        scratch_shapes=[
            pltpu.VMEM((3, ch, (band + 2) * cells), BF16),
            pltpu.VMEM((9, ch, ch), BF16),
        ],
        cost_estimate=work(grad, 1),
        compiler_params=pltpu.CompilerParams(vmem_limit_bytes=20 << 20),
        name="input",
    )(core, got, grad, outer, mine, theirs)


def exchange(block):
    return lax.ppermute(block, "core", [(0, 1), (1, 0)])


def across_chips(block):
    pairs = [(i, i + 1) for i in range(1, lax.axis_size(ROWS) - 1, 2)]
    return lax.ppermute(block, ROWS, pairs + [(b, a) for a, b in pairs])


def copies(block, axis):
    return jnp.broadcast_to(block[None], (lax.axis_size(axis), *block.shape))


def swap(parts, axis):
    return lax.all_to_all(parts, axis, 0, 0, tiled=True)


def total(parts):
    return lax.optimization_barrier(parts.astype(F32).sum(0))


def body(features, conv_weight, cotangent, valid_rows):
    band, ch, cells = features.shape
    images = cells // COLS
    near = conv_weight.shape[2]
    core = lax.axis_index("core").astype(jnp.int32)
    limits = lax.dynamic_slice_in_dim(valid_rows, lax.axis_index(CH) * images, images, 0)
    limits = limits - lax.axis_index(ROWS) * band
    where = core.reshape(1)
    shares = call_spread(where, conv_weight.reshape(9, near, ch), lax.axis_size(CH))
    inner = exchange(lax.dynamic_slice_in_dim(features, (1 - core) * (band - 1), 1, 0))
    outer = across_chips(lax.dynamic_slice_in_dim(features, core * (band - 1), 1, 0))
    mine = swap(shares, CH)
    theirs = exchange(mine)
    features, cotangent = call_stage(features, cotangent)
    grad_pre, outer_grad, own, sent = call_grad(
        limits, where, inner, features, outer, mine, theirs, cotangent
    )
    got = exchange(sent)
    outer_grad = across_chips(outer_grad)
    parts = own.shape[0]
    pair = (own + got[:parts].astype(F32)).astype(BF16)
    pair, inner_grad = lax.optimization_barrier((pair, got[parts:]))
    input_grad = call_input(where, inner_grad, grad_pre, outer_grad, mine, theirs)
    block = total(swap(pair, CH)).astype(BF16)
    block = call_sum(swap(copies(block, "z_near"), "z_near"), lax.axis_size("z_far"))
    block = swap(block, "z_far")
    mine = total(block)
    theirs = exchange(mine)
    weight_grad = call_join(where, mine, theirs).reshape(3, 3, near, ch)
    return input_grad, weight_grad


def solution(mesh):
    names = ("z_far", "z_near", "core", "ch_0", "ch_1")
    split = Mesh(mesh.devices.reshape(4, 4, 2, 4, 4), names)
    placed = (P(ROWS, None, CH), P(None, None, CH, None), P(ROWS, None, CH), P())
    return jax.shard_map(
        body,
        mesh=split,
        in_specs=placed,
        out_specs=(P(ROWS, None, CH), P(None, None, CH, None)),
        check_vma=False,
    )
```
